256 devices in a mesh: shot: 8 (over z), slab: 32 (over y, x, core).
Axes of the slice: x: 4, y: 4, z: 8, core: 2. Of those that a mesh axis runs over, the one named last changes fastest.
Arguments:
- source_field: bfloat16 [8, 256, 384, 512], P('shot', 'slab'), may hold values from -6 to 6
- receiver_fields: bfloat16 [16, 256, 384, 512], P('shot', 'slab'), may hold values from -6 to 6
- weights: int32 [16], P('shot'), may hold values from -1 to 1, as said below
- model: bfloat16 [256, 384, 512], P(('slab', 'shot')), may hold values from -6 to 6
- wedge_sizes: int32 [64], replicated, may hold values from 1 to 23, as said below
- wedge_scales: float32 [64], replicated, may hold values from 0.3 to 3
Outputs:
- new_model: float32 [256, 384, 512], P(('slab', 'shot'))
The draws below stay inside these ranges and needn't reach their ends.
Inputs may be any that keep to these rules, and one draw needn't show every extreme that they name: `weights`: each weight is -1 or +1. `wedge_sizes`: wedges 2d and 2d + 1 together hold either 512 // 32 // 2 or 24 columns, each count for half of the pairs; every wedge holds one column or more; all sizes sum to 512.
All inputs are finite; a program needn't handle non-finite values.
Results may differ from the reference program's by a relative error of at most 0.0003.
Values sent between devices are 32-bit elements; how exact they have to be, the bound alone decides.
No kernel may reach another device: no remote copies, remote signals or barrier semaphores. Data moves between devices by JAX's collectives and lax.ppermute only.
A program may use at most 128 MiB of HBM per device.

```python
import math
import jax
import jax.numpy as jnp
from jax import lax

NZ = 256
NY = 384
NX = 512
SH_DEV = 2
GROUPS = 8
SHOTS = 16
NWEDGE = 64
N_SHOT = 8
N_SLAB = 32


def draw_weights(key, part):
    return 2 * jax.random.randint(key, (SH_DEV * N_SHOT,), 0, 2, dtype=jnp.int32) - 1


def draw_wedge_sizes(key, part):
    first_key = jax.random.fold_in(key, 11)
    second_key = jax.random.fold_in(key, 23)
    share = NX // N_SLAB
    half = N_SLAB // 2
    pattern = jnp.concatenate([jnp.full((half,), share // 2, jnp.int32), jnp.full((N_SLAB - half,), 3 * share // 2, jnp.int32)])
    totals = pattern[jax.random.permutation(first_key, N_SLAB)]
    raw = jax.random.randint(second_key, (N_SLAB,), 0, 1 << 20, dtype=jnp.int32)
    leading = 1 + raw % jnp.maximum(totals - 1, 1)
    trailing = totals - leading
    return jnp.stack([leading, trailing], axis=1).reshape(-1).astype(jnp.int32)


def level_of(own_key, shape, shards, low, top_value):
    factor_of = 1.0
    for dim, shards_of in shards:
        draws = jax.random.uniform(jax.random.fold_in(jax.random.fold_in(own_key, 6), dim), (shards_of,), jnp.float32, low / len(shards), top_value / len(shards))
        factor_of = factor_of * jnp.repeat(jnp.exp(draws), shape[dim] // shards_of).reshape((-1,) + (1,) * (len(shape) - 1 - dim))
    return factor_of


def noise(stream_key, dims, width, bound, split=(), kind=jnp.bfloat16):
    gain = level_of(stream_key, dims, split, -0.22, 0.18) if split else 1.0
    drawn = jax.random.normal(stream_key, dims, jnp.float32) * width * gain
    return jnp.minimum(jnp.maximum(drawn, -bound), bound).astype(kind)


def setup_inputs(seed: int = 0) -> dict:
    keys = jax.random.split(jax.random.key(seed), 7)
    return {
        "source_field": noise(keys[0], (GROUPS, NZ, NY, NX), 1.0, 6.0, ((0, 8), (1, 32))),
        "receiver_fields": noise(keys[1], (SHOTS, NZ, NY, NX), 1.0, 6.0, ((0, 8), (1, 32))),
        "weights": draw_weights(jax.random.fold_in(keys[6], 71), 0),
        "model": noise(keys[3], (NZ, NY, NX), 1.0, 6.0, ((0, 256),)),
        "wedge_sizes": draw_wedge_sizes(jax.random.fold_in(keys[6], 71), 0),
        "wedge_scales": jnp.clip(jnp.exp(jax.random.uniform(keys[5], (NWEDGE,), jnp.float32, math.log(0.3), math.log(3.0))), 0.3, 3.0),
    }


STEP_SIZE = 0.25
EPSILON = 1e-06

def reference(source_field, receiver_fields, weights, model, wedge_sizes, wedge_scales):
    groups = source_field.shape[0]
    per_group = receiver_fields.shape[0] // groups
    signs = weights.astype(jnp.float32).reshape(groups, per_group)
    receivers = receiver_fields.reshape((groups, per_group) + receiver_fields.shape[1:])

    def add_group(total, inputs):
        source, group_fields, group_signs = inputs
        encoded = jnp.zeros(source.shape, jnp.float32)
        for member in range(per_group):
            encoded = encoded + group_signs[member] * group_fields[member].astype(jnp.float32)
        return (total + source.astype(jnp.float32) * encoded, None)
    gradient, _ = lax.scan(add_group, jnp.zeros(model.shape, jnp.float32), (source_field, receivers, signs))
    update = model.astype(jnp.float32) - STEP_SIZE * gradient
    spectrum = jnp.fft.fftn(update)
    depth, rows, columns = update.shape
    ends = jnp.cumsum(wedge_sizes).astype(jnp.int32)
    starts = (ends - wedge_sizes).astype(jnp.int32)
    column = jnp.arange(columns, dtype=jnp.int32)
    member_of = ((column[:, None] >= starts[None, :]) & (column[:, None] < ends[None, :])).astype(jnp.float32)
    energy = jnp.real(spectrum) ** 2 + jnp.imag(spectrum) ** 2
    column_power = lax.optimization_barrier(jnp.sum(energy, axis=(0, 1)))
    wedge_power = jnp.dot(column_power, member_of, precision=lax.Precision.HIGHEST)
    entries = wedge_sizes.astype(jnp.float32) * (depth * rows)
    spread = jnp.sqrt(wedge_power / entries + EPSILON)
    level = jnp.dot(member_of, wedge_scales * spread, precision=lax.Precision.HIGHEST)
    magnitude = jnp.sqrt(energy)
    factor = jnp.maximum(magnitude - level, 0.0) / jnp.maximum(magnitude, level)
    return jnp.real(jnp.fft.ifftn(spectrum * factor)).astype(jnp.float32)
```

```python
import functools

import jax
import jax.numpy as jnp
import numpy as np
from jax import lax
from jax.experimental import pallas as pl
from jax.experimental.pallas import tpu as pltpu
from jax.sharding import Mesh
from jax.sharding import PartitionSpec as P

SLAB = ("slab_0", "slab_1", "slab_2")
SLAB_SHOT = ("slab_0", "slab_1", "slab_2", "shot")

STEP_SIZE = 0.25
EPSILON = 1e-06
LANES = 128
F32 = jnp.float32
BF16 = jnp.bfloat16
INTERPRET = False


def halves(table):
    high = np.asarray(table, dtype=np.float32).astype(jnp.bfloat16)
    low = (np.asarray(table) - high.astype(np.float64)).astype(np.float32).astype(jnp.bfloat16)
    return jnp.asarray(high), jnp.asarray(low)


def angles(rows, columns, length):
    return 2.0 * np.pi * (np.outer(rows, columns) % length) / length


def x_table(width):
    half = width // 2
    angle = angles(np.arange(width), np.arange(half), width)
    sine = -np.sin(angle)
    sine[:, 0] = 1.0 - 2.0 * (np.arange(width) % 2)
    return np.concatenate([np.cos(angle), sine], axis=1)


def y_table(width):
    half = width // 2
    angle = angles(np.arange(half), np.arange(width), width)
    sine = np.sin(angle)
    sine[0] = 1.0 - 2.0 * (np.arange(width) % 2)
    return np.concatenate([np.cos(angle), sine], axis=0)


def y_back_table(width, shots, parts, rows):
    half = width // 2
    r, g, j = np.meshgrid(np.arange(rows), np.arange(parts), np.arange(shots), indexing="ij")
    ky = (j * (half // shots) + g * rows + r).reshape(-1)
    forward = y_table(width)
    return np.concatenate([forward[ky].T, forward[half + ky].T], axis=1)


def z_table(depth):
    angle = angles(np.arange(depth), np.arange(depth), depth)
    return np.concatenate([np.cos(angle), np.sin(angle)], axis=0)


def split(value):
    high = value.astype(BF16)
    low = (value - high.astype(F32)).astype(BF16)
    return high, low


def dot(a, b, dims=(((1,), (0,)), ((), ()))):
    return lax.dot_general(a, b, dims, preferred_element_type=F32)


def dot3(a, b, dims=(((1,), (0,)), ((), ()))):
    return dot(a[0], b[0], dims) + (dot(a[1], b[0], dims) + dot(a[0], b[1], dims))


def plane_kernel(
    shots, first, weight_ref, shot_ref, source_ref, receiver_ref, model_ref, xh_ref, xl_ref, yh_ref, yl_ref, out_ref
):
    plane = pl.program_id(0) + first
    members = receiver_ref.shape[0]
    encoded = weight_ref[0].astype(F32) * receiver_ref[0, 0].astype(F32)
    for member in range(1, members):
        encoded = encoded + weight_ref[member].astype(F32) * receiver_ref[member, 0].astype(F32)
    term = source_ref[0, 0].astype(F32) * encoded
    own = (plane == shot_ref[0]).astype(F32)
    term = own * model_ref[0].astype(F32) - STEP_SIZE * term
    along_x = dot3(split(term), (xh_ref[...], xl_ref[...]))
    both = dot3((yh_ref[...], yl_ref[...]), split(along_x))
    rows = both.shape[0] // 2
    half = both.shape[1] // 2
    cr, ci = both[:rows, :half], both[:rows, half:]
    sr, si = both[rows:, :half], both[rows:, half:]
    row = lax.broadcasted_iota(jnp.int32, (rows, half), 0)
    lane = lax.broadcasted_iota(jnp.int32, (rows, half), 1)
    row0 = row == 0
    lane0 = lane == 0
    edge = row0 | lane0
    pos_r = jnp.where(edge, cr, cr + si)
    pos_i = jnp.where(row0, ci, jnp.where(lane0, -sr, ci - sr))
    neg_r = jnp.where(row0, sr, jnp.where(lane0, ci, cr - si))
    neg_i = jnp.where(row0, si, jnp.where(lane0, -si, ci + sr))
    block = rows // shots
    for j in range(shots):
        part = slice(j * block, (j + 1) * block)
        out_ref[j, 0, 0, :block] = pos_r[part]
        out_ref[j, 0, 1, :block] = pos_i[part]
        out_ref[j, 0, 0, block:] = neg_r[part]
        out_ref[j, 0, 1, block:] = neg_i[part]


def plane_terms(weights, shot, source, receivers, model, tables, shots, first, count):
    _, planes, width_y, width_x = source.shape
    members = receivers.shape[0]
    xh, xl, yh, yl = tables
    whole = lambda a: pl.BlockSpec(a.shape, lambda p: (0,) * a.ndim)
    out_shape = (shots, count, 2, width_y // shots, width_x // 2)
    return pl.pallas_call(
        functools.partial(plane_kernel, shots, first),
        grid=(count,),
        in_specs=[
            pl.BlockSpec(memory_space=pltpu.SMEM),
            pl.BlockSpec(memory_space=pltpu.SMEM),
            pl.BlockSpec((1, 1, width_y, width_x), lambda p: (0, p + first, 0, 0)),
            pl.BlockSpec((members, 1, width_y, width_x), lambda p: (0, p + first, 0, 0)),
            whole(model),
            whole(xh),
            whole(xl),
            whole(yh),
            whole(yl),
        ],
        out_specs=pl.BlockSpec((shots, 1, 2, width_y // shots, width_x // 2), lambda p: (0, p, 0, 0, 0)),
        out_shape=jax.ShapeDtypeStruct(out_shape, F32),
        compiler_params=pltpu.CompilerParams(vmem_limit_bytes=48 * 1024 * 1024),
        cost_estimate=pl.CostEstimate(
            flops=count * 6 * width_y * width_x * (width_x + width_y),
            bytes_accessed=count * 10 * width_y * width_x,
            transcendentals=0,
        ),
        name="plane_terms",
        interpret=INTERPRET,
    )(weights, shot, source, receivers, model, xh, xl, yh, yl)


def pack_kernel(groups, shot_ref, in_ref, out_ref):
    planes, _, slots, half = in_ref.shape
    rows = slots // groups
    halves_x = half // LANES
    first = shot_ref[0] == 0
    lane0 = lax.broadcasted_iota(jnp.int32, (1, LANES), 1) == 0
    pos = [jnp.zeros((planes, LANES), F32) for _ in range(halves_x)]
    neg = [jnp.zeros((planes, LANES), F32) for _ in range(halves_x)]
    fix_a = jnp.zeros((planes, LANES), F32)
    fix_b = jnp.zeros((planes, LANES), F32)
    for slot in range(slots):
        g, r = divmod(slot, rows)
        for h in range(halves_x):
            real = in_ref[:, 0, slot, h * LANES : (h + 1) * LANES]
            imag = in_ref[:, 1, slot, h * LANES : (h + 1) * LANES]
            d = h * groups + g
            out_ref[d, r * planes : (r + 1) * planes] = real
            out_ref[d, (rows + r) * planes : (rows + r + 1) * planes] = imag
            real2, imag2 = real * real, imag * imag
            energy = real2 + imag2
            if h == 0 and slot in (0, slots // 2):
                fix_a = fix_a + real2
                fix_b = fix_b + imag2
                special = lane0 & first
                energy = jnp.where(special, 0.0, energy)
            if slot < slots // 2:
                pos[h] = pos[h] + energy
            else:
                neg[h] = neg[h] + energy
    keep = first.astype(F32)
    lines = []
    for h in range(halves_x):
        total = pos[h] + neg[h]
        if h == 0:
            lines.append(jnp.where(lane0, 2.0 * pos[0] + keep * fix_a, total))
        else:
            lines.append(total)
    for h in range(halves_x):
        total = pos[h] + neg[h]
        if h == 0:
            lines.append(jnp.where(lane0, 2.0 * neg[0] + keep * fix_b, total))
        else:
            lines.append(total)
    sums = jnp.concatenate([jnp.sum(line, axis=0, keepdims=True) for line in lines], axis=0)
    sums = jnp.concatenate([sums, jnp.zeros((8 - sums.shape[0], LANES), F32)], axis=0)
    base = 2 * rows * planes
    for d in range(halves_x * groups):
        out_ref[d, base : base + 8] = sums


def pack(shot, spectrum, groups):
    planes, _, slots, half = spectrum.shape
    rows = slots // groups
    out_shape = (groups * (half // LANES), 2 * rows * planes + 8, LANES)
    return pl.pallas_call(
        functools.partial(pack_kernel, groups),
        in_specs=[pl.BlockSpec(memory_space=pltpu.SMEM), pl.BlockSpec(memory_space=pltpu.VMEM)],
        out_specs=pl.BlockSpec(memory_space=pltpu.VMEM),
        out_shape=jax.ShapeDtypeStruct(out_shape, F32),
        name="pack",
        interpret=INTERPRET,
    )(shot, spectrum)


def levels_of(power, sizes, scales, cells):
    wedges = sizes.shape[1]
    down = lax.broadcasted_iota(jnp.int32, (wedges, wedges), 0)
    across = lax.broadcasted_iota(jnp.int32, (wedges, wedges), 1)
    size_row = jnp.broadcast_to(sizes.astype(F32), (wedges, wedges))
    scale_row = jnp.broadcast_to(scales, (wedges, wedges))
    ends = jnp.sum(jnp.where(across <= down, size_row, 0.0), axis=1, keepdims=True)
    size = jnp.sum(jnp.where(across == down, size_row, 0.0), axis=1, keepdims=True)
    scale = jnp.sum(jnp.where(across == down, scale_row, 0.0), axis=1, keepdims=True)
    starts = ends - size
    half_lines = power.shape[0] // 2
    half = half_lines * LANES
    members = []
    total = jnp.zeros((wedges, 1), F32)
    for line in range(2 * half_lines):
        base = (line % half_lines) * LANES
        column = lax.broadcasted_iota(jnp.int32, (wedges, LANES), 1) + base
        if line >= half_lines:
            column = jnp.where(column == 0, half, 2 * half - column)
        column = column.astype(F32)
        member = (column >= starts) & (column < ends)
        members.append(member)
        total = total + jnp.sum(jnp.where(member, power[line : line + 1], 0.0), axis=1, keepdims=True)
    spread = jnp.sqrt(total / (size * cells) + EPSILON)
    level = scale * spread
    return [jnp.sum(jnp.where(member, level, 0.0), axis=0, keepdims=True) for member in members]


def shrink_kernel(
    groups, cells, place_ref, in_ref, power_ref, sizes_ref, scales_ref, zh_ref, zl_ref, out_ref
):
    sources, message, _ = in_ref.shape
    depth = zh_ref.shape[1]
    planes = depth // sources
    rows = (message - 8) // (2 * planes)
    shot, slab = place_ref[0], place_ref[1]
    h, g = slab // groups, slab % groups
    lines = levels_of(power_ref[...] * depth, sizes_ref[...], scales_ref[...], cells)
    half_lines = len(lines) // 2
    own, mirror = lines[0], lines[half_lines]
    for other in range(1, half_lines):
        own = jnp.where(h == other, lines[other], own)
        mirror = jnp.where(h == other, lines[half_lines + other], mirror)
    lane = lax.broadcasted_iota(jnp.int32, (1, LANES), 1)
    edge = (lane == 0) & (h == 0)
    level_zero, level_mid = lines[0], lines[half_lines]
    upper = g >= groups // 2
    edge_level = jnp.where(upper, level_mid, level_zero)
    one = jnp.where(edge, edge_level, own)
    two = jnp.where(edge, edge_level, mirror)
    packed_here = (shot == 0) & (h == 0) & ((g == 0) | (g == groups // 2))
    packed = (lane == 0) & packed_here
    pieces = []
    for c in range(2):
        for r in range(rows):
            start = (c * rows + r) * planes
            pieces.append(in_ref[:, start : start + planes, :].reshape(depth, LANES))
    value = split(jnp.concatenate(pieces, axis=1))
    table = (zh_ref[...], zl_ref[...])
    both = dot3(table, value)
    shrunk_r, shrunk_i = [], []
    for r in range(rows):
        real = slice(r * LANES, (r + 1) * LANES)
        imag = slice((rows + r) * LANES, (rows + r + 1) * LANES)
        cr, sr = both[:depth, real], both[depth:, real]
        ci, si = both[:depth, imag], both[depth:, imag]
        zr, zi = cr + si, ci - sr
        energy = zr * zr + zi * zi
        if r == 0:
            energy_a = jnp.where(packed, cr * cr + sr * sr, energy)
            energy_b = jnp.where(packed, ci * ci + si * si, energy)
            one_a = jnp.where(packed, level_zero, one)
            two_a = jnp.where(packed, level_zero, two)
            one_b = jnp.where(packed, level_mid, one)
            two_b = jnp.where(packed, level_mid, two)
            factor_a = mean_factor(energy_a, one_a, two_a)
            factor_b = mean_factor(energy_b, one_b, two_b)
            shrunk_r.append(factor_a * cr + factor_b * si)
            shrunk_i.append(factor_b * ci - factor_a * sr)
        else:
            factor = mean_factor(energy, one, two)
            shrunk_r.append(factor * zr)
            shrunk_i.append(factor * zi)
    back = dot3(table, split(jnp.concatenate(shrunk_r + shrunk_i, axis=1)))
    wide = rows * LANES
    out_ref[:, 0, :wide] = back[:depth, :wide] - back[depth:, wide:]
    out_ref[:, 0, wide:] = back[:depth, wide:] + back[depth:, :wide]


def mean_factor(energy, one, two):
    magnitude = jnp.sqrt(energy)
    first = jnp.maximum(magnitude - one, 0.0) / jnp.maximum(magnitude, one)
    second = jnp.maximum(magnitude - two, 0.0) / jnp.maximum(magnitude, two)
    return 0.5 * (first + second)


def shrink(place, received, power, sizes, scales, tables, groups, cells):
    zh, zl = tables
    depth = zh.shape[1]
    planes = depth // received.shape[0]
    wide = (received.shape[1] - 8) // planes * LANES
    vmem = pl.BlockSpec(memory_space=pltpu.VMEM)
    return pl.pallas_call(
        functools.partial(shrink_kernel, groups, float(cells)),
        in_specs=[pl.BlockSpec(memory_space=pltpu.SMEM)] + [vmem] * 6,
        out_specs=vmem,
        out_shape=jax.ShapeDtypeStruct((depth, 1, wide), F32),
        name="shrink",
        interpret=INTERPRET,
    )(place, received, power, sizes, scales, zh, zl)


def image_kernel(groups, scale, in_ref, bh_ref, bl_ref, xh_ref, xl_ref, out_ref):
    count, _, wide = in_ref.shape
    rows = wide // (2 * LANES)
    halves_x = xh_ref.shape[1] // (2 * LANES)
    per_half = count // halves_x
    mid = per_half // 2
    row = lax.broadcasted_iota(jnp.int32, (mid, LANES), 0)
    lane = lax.broadcasted_iota(jnp.int32, (mid, LANES), 1)
    columns = [[], []]
    for h in range(halves_x):
        cos_r, cos_i, sin_r, sin_i = [], [], [], []
        for r in range(rows):
            real = slice(r * LANES, (r + 1) * LANES)
            imag = slice((rows + r) * LANES, (rows + r + 1) * LANES)
            low = slice(h * per_half, h * per_half + mid)
            high = slice(h * per_half + mid, (h + 1) * per_half)
            pr, pi = in_ref[low, 0, real], in_ref[low, 0, imag]
            nr, ni = in_ref[high, 0, real], in_ref[high, 0, imag]
            cr, ci, sr, si = pr + nr, pi + ni, ni - pi, pr - nr
            if h == 0:
                lane0 = lane == 0
                cr = jnp.where(lane0, 2.0 * pr, cr)
                ci = jnp.where(lane0, 2.0 * nr, ci)
                sr = jnp.where(lane0, -2.0 * pi, sr)
                si = jnp.where(lane0, -2.0 * ni, si)
            if r == 0:
                row0 = row == 0
                cr = jnp.where(row0, pr, cr)
                ci = jnp.where(row0, pi, ci)
                sr = jnp.where(row0, nr, sr)
                si = jnp.where(row0, ni, si)
            cos_r.append(cr)
            cos_i.append(ci)
            sin_r.append(sr)
            sin_i.append(si)
        columns[0].append(jnp.concatenate(cos_r + sin_r, axis=0))
        columns[1].append(jnp.concatenate(cos_i + sin_i, axis=0))
    stacked = jnp.concatenate(columns[0] + columns[1], axis=1)
    along_y = dot3((bh_ref[...], bl_ref[...]), split(stacked))
    lanes = lax.broadcasted_iota(jnp.int32, (1, along_y.shape[1]), 1)
    single = (lanes == 0) | (lanes == along_y.shape[1] // 2)
    along_y = along_y * jnp.where(single, scale, 2.0 * scale)
    out_ref[0] = dot3(split(along_y), (xh_ref[...], xl_ref[...]), (((1,), (1,)), ((), ())))


def image_of(returned, back_tables, x_tables, groups, scale, shape):
    vmem = pl.BlockSpec(memory_space=pltpu.VMEM)
    return pl.pallas_call(
        functools.partial(image_kernel, groups, scale),
        in_specs=[vmem] * 5,
        out_specs=vmem,
        out_shape=jax.ShapeDtypeStruct(shape, F32),
        name="image",
        interpret=INTERPRET,
    )(returned, *back_tables, *x_tables)


def on_device(source_field, receiver_fields, weights, model, wedge_sizes, wedge_scales):
    planes, width_y, width_x = source_field.shape[1:]
    shots = lax.axis_size("shot")
    slabs = lax.axis_size(SLAB)
    depth = planes * slabs
    groups = slabs // (width_x // 2 // LANES)
    rows = width_y // shots // groups
    shot = lax.axis_index("shot").astype(jnp.int32)
    slab = lax.axis_index(SLAB).astype(jnp.int32)
    x_tables = halves(x_table(width_x))
    y_tables = halves(y_table(width_y))
    z_tables = halves(z_table(depth))
    back_tables = halves(y_back_table(width_y, shots, groups // 2, rows))
    terms = plane_terms(
        weights, shot[None], source_field, receiver_fields, model, x_tables + y_tables, shots, 0, planes
    )
    summed = lax.psum_scatter(terms, "shot", scatter_dimension=0, tiled=True)[0]
    message = pack(shot[None], summed, groups)
    received = lax.all_to_all(message, SLAB, split_axis=0, concat_axis=0, tiled=True)
    lines = 2 * (width_x // 2 // LANES)
    base = 2 * rows * planes
    power = lax.psum(jnp.sum(received[:, base : base + lines, :], axis=0), "shot")
    shrunk = shrink(
        jnp.stack([shot, slab]),
        received,
        power,
        wedge_sizes[None],
        wedge_scales[None],
        z_tables,
        groups,
        depth * width_y,
    )
    returned = lax.all_to_all(shrunk, SLAB_SHOT, split_axis=0, concat_axis=0, tiled=True)
    scale = 1.0 / (depth * width_y * width_x)
    return image_of(returned, back_tables, x_tables, groups, scale, model.shape)


def solution(mesh):
    torus = Mesh(
        mesh.devices.reshape(mesh.shape["shot"], 4, 4, 2), ("shot", "slab_0", "slab_1", "slab_2")
    )
    return jax.shard_map(
        on_device,
        mesh=torus,
        in_specs=(
            P("shot", SLAB, None, None),
            P("shot", SLAB, None, None),
            P("shot"),
            P(SLAB_SHOT, None, None),
            P(),
            P(),
        ),
        out_specs=P(SLAB_SHOT, None, None),
        check_vma=False,
    )
```

```python
import functools

import jax
import jax.numpy as jnp
import numpy as np
from jax import lax
from jax.experimental import pallas as pl
from jax.experimental.pallas import tpu as pltpu
from jax.sharding import Mesh
from jax.sharding import PartitionSpec as P

SLAB = ("slab_0", "slab_1", "slab_2")
SLAB_SHOT = ("slab_0", "slab_1", "slab_2", "shot")

STEP_SIZE = 0.25
EPSILON = 1e-06
LANES = 128
F32 = jnp.float32
BF16 = jnp.bfloat16
INTERPRET = False
CHUNKS = 4
X_ROWS = 128
Y_ROWS = 96
ROOM = pltpu.CompilerParams(vmem_limit_bytes=24 * 1024 * 1024)


def halves(table):
    high = np.asarray(table, dtype=np.float32).astype(jnp.bfloat16)
    low = (np.asarray(table) - high.astype(np.float64)).astype(np.float32).astype(jnp.bfloat16)
    return jnp.asarray(high), jnp.asarray(low)


def angles(rows, columns, length):
    return 2.0 * np.pi * (np.outer(rows, columns) % length) / length


def x_table(width):
    half = width // 2
    angle = angles(np.arange(width), np.arange(half), width)
    sine = -np.sin(angle)
    sine[:, 0] = 1.0 - 2.0 * (np.arange(width) % 2)
    return np.concatenate([np.cos(angle), sine], axis=1)


def y_table(width):
    half = width // 2
    angle = angles(np.arange(half), np.arange(width), width)
    sine = np.sin(angle)
    sine[0] = 1.0 - 2.0 * (np.arange(width) % 2)
    return np.concatenate([np.cos(angle), sine], axis=0)


def y_back_table(width, shots, parts, rows):
    half = width // 2
    r, g, j = np.meshgrid(np.arange(rows), np.arange(parts), np.arange(shots), indexing="ij")
    ky = (j * (half // shots) + g * rows + r).reshape(-1)
    forward = y_table(width)
    return np.concatenate([forward[ky].T, forward[half + ky].T], axis=1)


def z_table(depth):
    angle = angles(np.arange(depth), np.arange(depth), depth)
    return np.concatenate([np.cos(angle), np.sin(angle)], axis=0)


def split(value):
    high = value.astype(BF16)
    low = (value - high.astype(F32)).astype(BF16)
    return high, low


def dot(a, b, dims=(((1,), (0,)), ((), ()))):
    return lax.dot_general(a, b, dims, preferred_element_type=F32)


def dot3(a, b, dims=(((1,), (0,)), ((), ()))):
    return dot(a[0], b[0], dims) + (dot(a[1], b[0], dims) + dot(a[0], b[1], dims))


def plane_kernel(
    shots, first, way, weight_ref, shot_ref, source_ref, receiver_ref, model_ref, xh_ref, xl_ref, yh_ref, yl_ref,
    start_ref, rest_ref, keep_ref, high_ref, low_ref
):
    plane = pl.program_id(0) + first
    members = receiver_ref.shape[0]
    own = (plane == shot_ref[0]).astype(F32)
    width_y = source_ref.shape[2]
    rows, half = width_y // 2, source_ref.shape[3] // 2
    signs = [weight_ref[member].astype(F32) for member in range(members)]

    @pl.loop(0, width_y // X_ROWS)
    def _(i):
        part = pl.ds(pl.multiple_of(i * X_ROWS, X_ROWS), X_ROWS)
        encoded = signs[0] * receiver_ref[0, 0, part].astype(F32)
        for member in range(1, members):
            encoded = encoded + signs[member] * receiver_ref[member, 0, part].astype(F32)
        term = source_ref[0, 0, part].astype(F32) * encoded
        term = own * model_ref[0, part].astype(F32) - STEP_SIZE * term
        along_x = split(dot3(split(term), (xh_ref[...], xl_ref[...])))
        high_ref[part] = along_x[0]
        low_ref[part] = along_x[1]

    @pl.loop(0, rows // Y_ROWS)
    def _(i):
        start = pl.multiple_of(i * Y_ROWS, Y_ROWS)
        part = pl.ds(start, Y_ROWS)
        other = pl.ds(pl.multiple_of(rows + i * Y_ROWS, Y_ROWS), Y_ROWS)
        value = (high_ref[...], low_ref[...])
        cos = dot3((yh_ref[part], yl_ref[part]), value)
        sin = dot3((yh_ref[other], yl_ref[other]), value)
        cr, ci, sr, si = cos[:, :half], cos[:, half:], sin[:, :half], sin[:, half:]
        row = lax.broadcasted_iota(jnp.int32, (Y_ROWS, half), 0) + start
        lane = lax.broadcasted_iota(jnp.int32, (Y_ROWS, half), 1)
        row0 = row == 0
        lane0 = lane == 0
        edge = row0 | lane0
        keep_ref[0, part] = jnp.where(edge, cr, cr + si)
        keep_ref[1, part] = jnp.where(row0, ci, jnp.where(lane0, -sr, ci - sr))
        keep_ref[2, part] = jnp.where(row0, sr, jnp.where(lane0, ci, cr - si))
        keep_ref[3, part] = jnp.where(row0, si, jnp.where(lane0, -si, ci + sr))

    block = rows // shots
    for order in range(shots):
        owner = lax.rem(shot_ref[0] + 2 * shots - way * (1 + order), shots)
        part = pl.ds(pl.multiple_of(owner * block, 8), block)
        target = start_ref.at[0] if order == 0 else rest_ref.at[order - 1, 0]
        target[0, :block] = keep_ref[0, part]
        target[1, :block] = keep_ref[1, part]
        target[0, block:] = keep_ref[2, part]
        target[1, block:] = keep_ref[3, part]


def plane_terms(weights, shot, source, receivers, model, tables, shots, first, count, way):
    _, planes, width_y, width_x = source.shape
    members = receivers.shape[0]
    xh, xl, yh, yl = tables
    whole = lambda a: pl.BlockSpec(a.shape, lambda p: (0,) * a.ndim)
    piece = (2, width_y // shots, width_x // 2)
    return pl.pallas_call(
        functools.partial(plane_kernel, shots, first, way),
        grid=(count,),
        in_specs=[
            pl.BlockSpec(memory_space=pltpu.SMEM),
            pl.BlockSpec(memory_space=pltpu.SMEM),
            pl.BlockSpec((1, 1, width_y, width_x), lambda p: (0, p + first, 0, 0)),
            pl.BlockSpec((members, 1, width_y, width_x), lambda p: (0, p + first, 0, 0)),
            whole(model),
            whole(xh),
            whole(xl),
            whole(yh),
            whole(yl),
        ],
        out_specs=[
            pl.BlockSpec((1,) + piece, lambda p: (p, 0, 0, 0)),
            pl.BlockSpec((shots - 1, 1) + piece, lambda p: (0, p, 0, 0, 0)),
        ],
        out_shape=[
            jax.ShapeDtypeStruct((count,) + piece, F32),
            jax.ShapeDtypeStruct((shots - 1, count) + piece, F32),
        ],
        scratch_shapes=[
            pltpu.VMEM((4, width_y // 2, width_x // 2), F32),
            pltpu.VMEM((width_y, width_x), BF16),
            pltpu.VMEM((width_y, width_x), BF16),
        ],
        cost_estimate=pl.CostEstimate(
            flops=count * 6 * width_y * width_x * (width_x + width_y),
            bytes_accessed=count * 10 * width_y * width_x,
            transcendentals=0,
        ),
        name="plane_terms",
        interpret=INTERPRET,
    )(weights, shot, source, receivers, model, xh, xl, yh, yl)


def pack_kernel(groups, chunks, shot_ref, *refs):
    ins, out_ref = refs[: 2 * chunks], refs[2 * chunks]
    planes = sum(ref.shape[0] for ref in ins[:chunks])
    _, _, slots, half = ins[0].shape
    rows = slots // groups
    halves_x = half // LANES
    first = shot_ref[0] == 0
    lane0 = lax.broadcasted_iota(jnp.int32, (1, LANES), 1) == 0

    def plane_lines(c, slot, h):
        lanes = slice(h * LANES, (h + 1) * LANES)
        parts = [
            came[:, c, slot, lanes] + last[0, :, c, slot, lanes]
            for came, last in zip(ins[:chunks], ins[chunks:])
        ]
        return jnp.concatenate(parts, axis=0)

    pos = [jnp.zeros((planes, LANES), F32) for _ in range(halves_x)]
    neg = [jnp.zeros((planes, LANES), F32) for _ in range(halves_x)]
    fix_a = jnp.zeros((planes, LANES), F32)
    fix_b = jnp.zeros((planes, LANES), F32)
    for slot in range(slots):
        g, r = divmod(slot, rows)
        for h in range(halves_x):
            real = plane_lines(0, slot, h)
            imag = plane_lines(1, slot, h)
            d = h * groups + g
            out_ref[d, r * planes : (r + 1) * planes] = real
            out_ref[d, (rows + r) * planes : (rows + r + 1) * planes] = imag
            real2, imag2 = real * real, imag * imag
            energy = real2 + imag2
            if h == 0 and slot in (0, slots // 2):
                fix_a = fix_a + real2
                fix_b = fix_b + imag2
                special = lane0 & first
                energy = jnp.where(special, 0.0, energy)
            if slot < slots // 2:
                pos[h] = pos[h] + energy
            else:
                neg[h] = neg[h] + energy
    keep = first.astype(F32)
    lines = []
    for side, fix in ((pos, fix_a), (neg, fix_b)):
        for h in range(halves_x):
            total = pos[h] + neg[h]
            lines.append(jnp.where(lane0, 2.0 * side[0] + keep * fix, total) if h == 0 else total)
    sums = jnp.concatenate([jnp.sum(line, axis=0, keepdims=True) for line in lines], axis=0)
    sums = jnp.concatenate([sums, jnp.zeros((8 - sums.shape[0], LANES), F32)], axis=0)
    base = 2 * rows * planes
    for d in range(halves_x * groups):
        out_ref[d, base : base + 8] = sums


def pack(shot, came, rests, groups):
    chunks = len(came)
    planes = sum(a.shape[0] for a in came)
    _, _, slots, half = came[0].shape
    rows = slots // groups
    out_shape = (groups * (half // LANES), 2 * rows * planes + 8, LANES)
    return pl.pallas_call(
        functools.partial(pack_kernel, groups, chunks),
        grid=(1,),
        in_specs=[pl.BlockSpec(memory_space=pltpu.SMEM)]
        + [pl.BlockSpec(a.shape, lambda i: (0, 0, 0, 0)) for a in came]
        + [pl.BlockSpec((1,) + a.shape[1:], lambda i, last=a.shape[0] - 1: (last, 0, 0, 0, 0)) for a in rests],
        out_specs=pl.BlockSpec(out_shape, lambda i: (0, 0, 0)),
        out_shape=jax.ShapeDtypeStruct(out_shape, F32),
        cost_estimate=pl.CostEstimate(flops=10**9, bytes_accessed=10**6, transcendentals=0),
        compiler_params=ROOM,
        name="pack",
        interpret=INTERPRET,
    )(shot, *came, *rests)


def levels_of(power, sizes, scales, cells):
    wedges = sizes.shape[1]
    down = lax.broadcasted_iota(jnp.int32, (wedges, wedges), 0)
    across = lax.broadcasted_iota(jnp.int32, (wedges, wedges), 1)
    size_row = jnp.broadcast_to(sizes.astype(F32), (wedges, wedges))
    scale_row = jnp.broadcast_to(scales, (wedges, wedges))
    ends = jnp.sum(jnp.where(across <= down, size_row, 0.0), axis=1, keepdims=True)
    size = jnp.sum(jnp.where(across == down, size_row, 0.0), axis=1, keepdims=True)
    scale = jnp.sum(jnp.where(across == down, scale_row, 0.0), axis=1, keepdims=True)
    starts = ends - size
    half_lines = power.shape[0] // 2
    half = half_lines * LANES
    members = []
    total = jnp.zeros((wedges, 1), F32)
    for line in range(2 * half_lines):
        base = (line % half_lines) * LANES
        column = lax.broadcasted_iota(jnp.int32, (wedges, LANES), 1) + base
        if line >= half_lines:
            column = jnp.where(column == 0, half, 2 * half - column)
        column = column.astype(F32)
        member = (column >= starts) & (column < ends)
        members.append(member)
        total = total + jnp.sum(jnp.where(member, power[line : line + 1], 0.0), axis=1, keepdims=True)
    spread = jnp.sqrt(total / (size * cells) + EPSILON)
    level = scale * spread
    return [jnp.sum(jnp.where(member, level, 0.0), axis=0, keepdims=True) for member in members]


def shrink_kernel(
    groups, cells, place_ref, in_ref, power_ref, sizes_ref, scales_ref, zh_ref, zl_ref, out_ref
):
    sources, message, _ = in_ref.shape
    depth = zh_ref.shape[1]
    planes = depth // sources
    rows = (message - 8) // (2 * planes)
    shot, slab = place_ref[0], place_ref[1]
    h, g = slab // groups, slab % groups
    lines = levels_of(power_ref[: 2 * (sources // groups)] * depth, sizes_ref[...], scales_ref[...], cells)
    half_lines = len(lines) // 2
    own, mirror = lines[0], lines[half_lines]
    for other in range(1, half_lines):
        own = jnp.where(h == other, lines[other], own)
        mirror = jnp.where(h == other, lines[half_lines + other], mirror)
    lane = lax.broadcasted_iota(jnp.int32, (1, LANES), 1)
    edge = (lane == 0) & (h == 0)
    level_zero, level_mid = lines[0], lines[half_lines]
    upper = g >= groups // 2
    edge_level = jnp.where(upper, level_mid, level_zero)
    one = jnp.where(edge, edge_level, own)
    two = jnp.where(edge, edge_level, mirror)
    packed_here = (shot == 0) & (h == 0) & ((g == 0) | (g == groups // 2))
    packed = (lane == 0) & packed_here
    pieces = []
    for c in range(2):
        for r in range(rows):
            start = (c * rows + r) * planes
            pieces.append(in_ref[:, start : start + planes, :].reshape(depth, LANES))
    value = split(jnp.concatenate(pieces, axis=1))
    table = (zh_ref[...], zl_ref[...])
    both = dot3(table, value)
    shrunk_r, shrunk_i = [], []
    for r in range(rows):
        real = slice(r * LANES, (r + 1) * LANES)
        imag = slice((rows + r) * LANES, (rows + r + 1) * LANES)
        cr, sr = both[:depth, real], both[depth:, real]
        ci, si = both[:depth, imag], both[depth:, imag]
        zr, zi = cr + si, ci - sr
        energy = zr * zr + zi * zi
        if r == 0:
            energy_a = jnp.where(packed, cr * cr + sr * sr, energy)
            energy_b = jnp.where(packed, ci * ci + si * si, energy)
            one_a = jnp.where(packed, level_zero, one)
            two_a = jnp.where(packed, level_zero, two)
            one_b = jnp.where(packed, level_mid, one)
            two_b = jnp.where(packed, level_mid, two)
            factor_a = mean_factor(energy_a, one_a, two_a)
            factor_b = mean_factor(energy_b, one_b, two_b)
            shrunk_r.append(factor_a * cr + factor_b * si)
            shrunk_i.append(factor_b * ci - factor_a * sr)
        else:
            factor = mean_factor(energy, one, two)
            shrunk_r.append(factor * zr)
            shrunk_i.append(factor * zi)
    back = dot3(table, split(jnp.concatenate(shrunk_r + shrunk_i, axis=1)))
    wide = rows * LANES
    out_ref[:, 0, :wide] = back[:depth, :wide] - back[depth:, wide:]
    out_ref[:, 0, wide:] = back[:depth, wide:] + back[depth:, :wide]


def mean_factor(energy, one, two):
    magnitude = jnp.sqrt(energy)
    first = jnp.maximum(magnitude - one, 0.0) / jnp.maximum(magnitude, one)
    second = jnp.maximum(magnitude - two, 0.0) / jnp.maximum(magnitude, two)
    return 0.5 * (first + second)


def shrink(place, received, power, sizes, scales, tables, groups, cells):
    zh, zl = tables
    depth = zh.shape[1]
    planes = depth // received.shape[0]
    wide = (received.shape[1] - 8) // planes * LANES
    vmem = pl.BlockSpec(memory_space=pltpu.VMEM)
    return pl.pallas_call(
        functools.partial(shrink_kernel, groups, float(cells)),
        in_specs=[pl.BlockSpec(memory_space=pltpu.SMEM)] + [vmem] * 6,
        out_specs=vmem,
        out_shape=jax.ShapeDtypeStruct((depth, 1, wide), F32),
        compiler_params=ROOM,
        name="shrink",
        interpret=INTERPRET,
    )(place, received, power, sizes, scales, zh, zl)


def image_kernel(groups, scale, in_ref, bh_ref, bl_ref, xh_ref, xl_ref, out_ref):
    count, _, wide = in_ref.shape
    rows = wide // (2 * LANES)
    halves_x = xh_ref.shape[1] // (2 * LANES)
    per_half = count // halves_x
    mid = per_half // 2
    row = lax.broadcasted_iota(jnp.int32, (mid, LANES), 0)
    lane = lax.broadcasted_iota(jnp.int32, (mid, LANES), 1)
    columns = [[], []]
    for h in range(halves_x):
        cos_r, cos_i, sin_r, sin_i = [], [], [], []
        for r in range(rows):
            real = slice(r * LANES, (r + 1) * LANES)
            imag = slice((rows + r) * LANES, (rows + r + 1) * LANES)
            low = slice(h * per_half, h * per_half + mid)
            high = slice(h * per_half + mid, (h + 1) * per_half)
            pr, pi = in_ref[low, 0, real], in_ref[low, 0, imag]
            nr, ni = in_ref[high, 0, real], in_ref[high, 0, imag]
            cr, ci, sr, si = pr + nr, pi + ni, ni - pi, pr - nr
            if h == 0:
                lane0 = lane == 0
                cr = jnp.where(lane0, 2.0 * pr, cr)
                ci = jnp.where(lane0, 2.0 * nr, ci)
                sr = jnp.where(lane0, -2.0 * pi, sr)
                si = jnp.where(lane0, -2.0 * ni, si)
            if r == 0:
                row0 = row == 0
                cr = jnp.where(row0, pr, cr)
                ci = jnp.where(row0, pi, ci)
                sr = jnp.where(row0, nr, sr)
                si = jnp.where(row0, ni, si)
            cos_r.append(cr)
            cos_i.append(ci)
            sin_r.append(sr)
            sin_i.append(si)
        columns[0].append(jnp.concatenate(cos_r + sin_r, axis=0))
        columns[1].append(jnp.concatenate(cos_i + sin_i, axis=0))
    stacked = jnp.concatenate(columns[0] + columns[1], axis=1)
    along_y = dot3((bh_ref[...], bl_ref[...]), split(stacked))
    lanes = lax.broadcasted_iota(jnp.int32, (1, along_y.shape[1]), 1)
    single = (lanes == 0) | (lanes == along_y.shape[1] // 2)
    along_y = along_y * jnp.where(single, scale, 2.0 * scale)
    out_ref[0] = dot3(split(along_y), (xh_ref[...], xl_ref[...]), (((1,), (1,)), ((), ())))


def image_of(returned, back_tables, x_tables, groups, scale, shape):
    vmem = pl.BlockSpec(memory_space=pltpu.VMEM)
    return pl.pallas_call(
        functools.partial(image_kernel, groups, scale),
        in_specs=[vmem] * 5,
        out_specs=vmem,
        out_shape=jax.ShapeDtypeStruct(shape, F32),
        compiler_params=ROOM,
        name="image",
        interpret=INTERPRET,
    )(returned, *back_tables, *x_tables)


def on_device(source_field, receiver_fields, weights, model, wedge_sizes, wedge_scales):
    planes, width_y, width_x = source_field.shape[1:]
    shots = lax.axis_size("shot")
    slabs = lax.axis_size(SLAB)
    depth = planes * slabs
    groups = slabs // (width_x // 2 // LANES)
    rows = width_y // shots // groups
    shot = lax.axis_index("shot").astype(jnp.int32)
    slab = lax.axis_index(SLAB).astype(jnp.int32)
    x_tables = halves(x_table(width_x))
    y_tables = halves(y_table(width_y))
    z_tables = halves(z_table(depth))
    back_tables = halves(y_back_table(width_y, shots, groups // 2, rows))
    chunk = planes // CHUNKS
    came, rests = [], []
    for q in range(CHUNKS):
        way = 1 - 2 * (q % 2)
        start, rest = plane_terms(
            weights, shot[None], source_field, receiver_fields, model, x_tables + y_tables,
            shots, q * chunk, chunk, way,
        )
        came.append(start)
        rests.append(rest)
    for step in range(shots - 1):
        for q in range(CHUNKS):
            way = 1 - 2 * (q % 2)
            moved = lax.ppermute(came[q], "shot", [(i, (i + way) % shots) for i in range(shots)])
            came[q] = moved if step == shots - 2 else moved + rests[q][step]
    message = pack(shot[None], came, rests, groups)
    received = lax.all_to_all(message, SLAB, split_axis=0, concat_axis=0, tiled=True)
    base = 2 * rows * planes
    power = jnp.sum(received[:, base:, :], axis=0)
    for part in [
        lax.ppermute(power, "shot", [(i, (i + k) % shots) for i in range(shots)]) for k in range(1, shots)
    ]:
        power = power + part
    shrunk = shrink(
        jnp.stack([shot, slab]),
        received,
        power,
        wedge_sizes[None],
        wedge_scales[None],
        z_tables,
        groups,
        depth * width_y,
    )
    returned = lax.all_to_all(shrunk, SLAB_SHOT, split_axis=0, concat_axis=0, tiled=True)
    scale = 1.0 / (depth * width_y * width_x)
    return image_of(returned, back_tables, x_tables, groups, scale, model.shape)


def solution(mesh):
    torus = Mesh(
        mesh.devices.reshape(mesh.shape["shot"], 4, 4, 2), ("shot", "slab_0", "slab_1", "slab_2")
    )
    return jax.shard_map(
        on_device,
        mesh=torus,
        in_specs=(
            P("shot", SLAB, None, None),
            P("shot", SLAB, None, None),
            P("shot"),
            P(SLAB_SHOT, None, None),
            P(),
            P(),
        ),
        out_specs=P(SLAB_SHOT, None, None),
        check_vma=False,
    )
```

```python
import functools

import jax
import jax.numpy as jnp
import numpy as np
from jax import lax
from jax.experimental import pallas as pl
from jax.experimental.pallas import tpu as pltpu
from jax.sharding import Mesh
from jax.sharding import PartitionSpec as P

SLAB = ("slab_0", "slab_1", "slab_2")
SLAB_SHOT = ("slab_0", "slab_1", "slab_2", "shot")

STEP_SIZE = 0.25
EPSILON = 1e-06
LANES = 128
F32 = jnp.float32
BF16 = jnp.bfloat16
INTERPRET = False
CHUNKS = 4
ROOM = pltpu.CompilerParams(vmem_limit_bytes=24 * 1024 * 1024)


def halves(table):
    high = np.asarray(table, dtype=np.float32).astype(jnp.bfloat16)
    low = (np.asarray(table) - high.astype(np.float64)).astype(np.float32).astype(jnp.bfloat16)
    return jnp.asarray(high), jnp.asarray(low)


def angles(rows, columns, length):
    return 2.0 * np.pi * (np.outer(rows, columns) % length) / length


def x_table(width):
    half = width // 2
    tables = []
    for h in range(2):
        angle = angles(np.arange(half), np.arange(h, half, 2), width)
        sine = -np.sin(angle)
        if h == 0:
            sine[:, 0] = 1.0 - 2.0 * (np.arange(half) % 2)
        tables.append(np.concatenate([np.cos(angle), sine], axis=1))
    return np.stack(tables)


def y_order(width):
    half = width // 2
    return np.concatenate([np.arange(0, half, 2), np.arange(1, half, 2)])


def y_rows(width, length):
    angle = angles(y_order(width), np.arange(length), width)
    sine = np.sin(angle)
    sine[0] = 1.0 - 2.0 * (np.arange(length) % 2)
    return np.cos(angle), sine


def y_table(width):
    cos, sin = y_rows(width, width // 2)
    quarter = width // 4
    return np.stack(
        [np.concatenate([cos[part], sin[part]]) for part in (slice(0, quarter), slice(quarter, None))]
    )


def y_back_table(width, shots, parts, rows):
    half = width // 2
    r, g, j = np.meshgrid(np.arange(rows), np.arange(parts), np.arange(shots), indexing="ij")
    slot = (j * (half // shots) + g * rows + r).reshape(-1)
    cos, sin = y_rows(width, width)
    return np.concatenate([cos[slot].T, sin[slot].T], axis=1)


def z_table(depth):
    angle = angles(np.arange(depth), np.arange(depth), depth)
    return np.concatenate([np.cos(angle), np.sin(angle)], axis=0)


def split(value):
    high = value.astype(BF16)
    low = (value - high.astype(F32)).astype(BF16)
    return high, low


def dot(a, b, dims=(((1,), (0,)), ((), ()))):
    return lax.dot_general(a, b, dims, preferred_element_type=F32)


def dot3(a, b, dims=(((1,), (0,)), ((), ()))):
    return dot(a[0], b[0], dims) + (dot(a[1], b[0], dims) + dot(a[0], b[1], dims))


def plane_kernel(
    shots, first, way, weight_ref, shot_ref, source_ref, receiver_ref, model_ref, xh_ref, xl_ref, yh_ref, yl_ref,
    start_ref, rest_ref, keep_ref
):
    plane = pl.program_id(0) + first
    members = receiver_ref.shape[0]
    own = (plane == shot_ref[0]).astype(F32)
    width_y, width_x = source_ref.shape[2:]
    rows, half = width_y // 2, width_x // 2
    encoded = weight_ref[0].astype(F32) * receiver_ref[0, 0].astype(F32)
    for member in range(1, members):
        encoded = encoded + weight_ref[member].astype(F32) * receiver_ref[member, 0].astype(F32)
    term = source_ref[0, 0].astype(F32) * encoded
    term = own * model_ref[0].astype(F32) - STEP_SIZE * term
    low, high = term[:, :half], term[:, half:]
    cosines, sines = [], []
    for h, fold in ((0, low + high), (1, low - high)):
        fold = jnp.concatenate([fold[:rows] + fold[rows:], fold[:rows] - fold[rows:]], axis=0)
        along_x = dot3(split(fold), (xh_ref[h], xl_ref[h]))
        cosines.append(along_x[:, : half // 2])
        sines.append(along_x[:, half // 2 :])
    along_x = jnp.concatenate(cosines + sines, axis=1)
    quarter = rows // 2
    row = lax.broadcasted_iota(jnp.int32, (quarter, half), 0)
    lane0 = lax.broadcasted_iota(jnp.int32, (quarter, half), 1) == 0
    for parity in range(2):
        both = dot3((yh_ref[parity], yl_ref[parity]), split(along_x[parity * rows : (parity + 1) * rows]))
        cr, ci = both[:quarter, :half], both[:quarter, half:]
        sr, si = both[quarter:, :half], both[quarter:, half:]
        part = pl.ds(parity * quarter, quarter)
        if parity == 0:
            row0 = row == 0
            keep_ref[0, part] = jnp.where(row0 | lane0, cr, cr + si)
            keep_ref[1, part] = jnp.where(row0, ci, jnp.where(lane0, -sr, ci - sr))
            keep_ref[2, part] = jnp.where(row0, sr, jnp.where(lane0, ci, cr - si))
            keep_ref[3, part] = jnp.where(row0, si, jnp.where(lane0, -si, ci + sr))
        else:
            keep_ref[0, part] = jnp.where(lane0, cr, cr + si)
            keep_ref[1, part] = jnp.where(lane0, -sr, ci - sr)
            keep_ref[2, part] = jnp.where(lane0, ci, cr - si)
            keep_ref[3, part] = jnp.where(lane0, -si, ci + sr)
    block = rows // shots
    for order in range(shots):
        owner = lax.rem(shot_ref[0] + 2 * shots - way * (1 + order), shots)
        part = pl.ds(pl.multiple_of(owner * block, 8), block)
        target = start_ref.at[0] if order == 0 else rest_ref.at[order - 1, 0]
        target[0, :block] = keep_ref[0, part]
        target[1, :block] = keep_ref[1, part]
        target[0, block:] = keep_ref[2, part]
        target[1, block:] = keep_ref[3, part]


def plane_terms(weights, shot, source, receivers, model, tables, shots, first, count, way):
    _, planes, width_y, width_x = source.shape
    members = receivers.shape[0]
    xh, xl, yh, yl = tables
    whole = lambda a: pl.BlockSpec(a.shape, lambda p: (0,) * a.ndim)
    piece = (2, width_y // shots, width_x // 2)
    return pl.pallas_call(
        functools.partial(plane_kernel, shots, first, way),
        grid=(count,),
        in_specs=[
            pl.BlockSpec(memory_space=pltpu.SMEM),
            pl.BlockSpec(memory_space=pltpu.SMEM),
            pl.BlockSpec((1, 1, width_y, width_x), lambda p: (0, p + first, 0, 0)),
            pl.BlockSpec((members, 1, width_y, width_x), lambda p: (0, p + first, 0, 0)),
            whole(model),
            whole(xh),
            whole(xl),
            whole(yh),
            whole(yl),
        ],
        out_specs=[
            pl.BlockSpec((1,) + piece, lambda p: (p, 0, 0, 0)),
            pl.BlockSpec((shots - 1, 1) + piece, lambda p: (0, p, 0, 0, 0)),
        ],
        out_shape=[
            jax.ShapeDtypeStruct((count,) + piece, F32),
            jax.ShapeDtypeStruct((shots - 1, count) + piece, F32),
        ],
        scratch_shapes=[pltpu.VMEM((4, width_y // 2, width_x // 2), F32)],
        cost_estimate=pl.CostEstimate(
            flops=count * 3 * width_y * width_x * (width_x + width_y),
            bytes_accessed=count * 10 * width_y * width_x,
            transcendentals=0,
        ),
        name="plane_terms",
        interpret=INTERPRET,
    )(weights, shot, source, receivers, model, xh, xl, yh, yl)


def pack_kernel(groups, chunks, shot_ref, *refs):
    ins, out_ref = refs[: 2 * chunks], refs[2 * chunks]
    planes = sum(ref.shape[0] for ref in ins[:chunks])
    _, _, slots, half = ins[0].shape
    rows = slots // groups
    halves_x = half // LANES
    first = shot_ref[0] == 0
    lane0 = lax.broadcasted_iota(jnp.int32, (1, LANES), 1) == 0

    def plane_lines(c, slot, h):
        lanes = slice(h * LANES, (h + 1) * LANES)
        parts = [
            came[:, c, slot, lanes] + last[0, :, c, slot, lanes]
            for came, last in zip(ins[:chunks], ins[chunks:])
        ]
        return jnp.concatenate(parts, axis=0)

    pos = [jnp.zeros((planes, LANES), F32) for _ in range(halves_x)]
    neg = [jnp.zeros((planes, LANES), F32) for _ in range(halves_x)]
    fix_a = jnp.zeros((planes, LANES), F32)
    fix_b = jnp.zeros((planes, LANES), F32)
    for slot in range(slots):
        g, r = divmod(slot, rows)
        for h in range(halves_x):
            real = plane_lines(0, slot, h)
            imag = plane_lines(1, slot, h)
            d = h * groups + g
            out_ref[d, r * planes : (r + 1) * planes] = real
            out_ref[d, (rows + r) * planes : (rows + r + 1) * planes] = imag
            real2, imag2 = real * real, imag * imag
            energy = real2 + imag2
            if h == 0 and slot in (0, slots // 2):
                fix_a = fix_a + real2
                fix_b = fix_b + imag2
                special = lane0 & first
                energy = jnp.where(special, 0.0, energy)
            if slot < slots // 2:
                pos[h] = pos[h] + energy
            else:
                neg[h] = neg[h] + energy
    keep = first.astype(F32)
    lines = []
    for side, fix in ((pos, fix_a), (neg, fix_b)):
        for h in range(halves_x):
            total = pos[h] + neg[h]
            lines.append(jnp.where(lane0, 2.0 * side[0] + keep * fix, total) if h == 0 else total)
    sums = jnp.concatenate([jnp.sum(line, axis=0, keepdims=True) for line in lines], axis=0)
    sums = jnp.concatenate([sums, jnp.zeros((8 - sums.shape[0], LANES), F32)], axis=0)
    base = 2 * rows * planes
    for d in range(halves_x * groups):
        out_ref[d, base : base + 8] = sums


def pack(shot, came, rests, groups):
    chunks = len(came)
    planes = sum(a.shape[0] for a in came)
    _, _, slots, half = came[0].shape
    rows = slots // groups
    out_shape = (groups * (half // LANES), 2 * rows * planes + 8, LANES)
    return pl.pallas_call(
        functools.partial(pack_kernel, groups, chunks),
        grid=(1,),
        in_specs=[pl.BlockSpec(memory_space=pltpu.SMEM)]
        + [pl.BlockSpec(a.shape, lambda i: (0, 0, 0, 0)) for a in came]
        + [pl.BlockSpec((1,) + a.shape[1:], lambda i, last=a.shape[0] - 1: (last, 0, 0, 0, 0)) for a in rests],
        out_specs=pl.BlockSpec(out_shape, lambda i: (0, 0, 0)),
        out_shape=jax.ShapeDtypeStruct(out_shape, F32),
        cost_estimate=pl.CostEstimate(flops=10**9, bytes_accessed=10**6, transcendentals=0),
        compiler_params=ROOM,
        name="pack",
        interpret=INTERPRET,
    )(shot, *came, *rests)


def levels_of(power, sizes, scales, cells):
    wedges = sizes.shape[1]
    down = lax.broadcasted_iota(jnp.int32, (wedges, wedges), 0)
    across = lax.broadcasted_iota(jnp.int32, (wedges, wedges), 1)
    size_row = jnp.broadcast_to(sizes.astype(F32), (wedges, wedges))
    scale_row = jnp.broadcast_to(scales, (wedges, wedges))
    ends = jnp.sum(jnp.where(across <= down, size_row, 0.0), axis=1, keepdims=True)
    size = jnp.sum(jnp.where(across == down, size_row, 0.0), axis=1, keepdims=True)
    scale = jnp.sum(jnp.where(across == down, scale_row, 0.0), axis=1, keepdims=True)
    starts = ends - size
    half_lines = power.shape[0] // 2
    half = half_lines * LANES
    members = []
    total = jnp.zeros((wedges, 1), F32)
    for line in range(2 * half_lines):
        column = half_lines * lax.broadcasted_iota(jnp.int32, (wedges, LANES), 1) + line % half_lines
        if line >= half_lines:
            column = jnp.where(column == 0, half, 2 * half - column)
        column = column.astype(F32)
        member = (column >= starts) & (column < ends)
        members.append(member)
        total = total + jnp.sum(jnp.where(member, power[line : line + 1], 0.0), axis=1, keepdims=True)
    spread = jnp.sqrt(total / (size * cells) + EPSILON)
    level = scale * spread
    return [jnp.sum(jnp.where(member, level, 0.0), axis=0, keepdims=True) for member in members]


def shrink_kernel(
    groups, cells, place_ref, in_ref, power_ref, sizes_ref, scales_ref, zh_ref, zl_ref, out_ref
):
    sources, message, _ = in_ref.shape
    depth = zh_ref.shape[1]
    planes = depth // sources
    rows = (message - 8) // (2 * planes)
    shot, slab = place_ref[0], place_ref[1]
    h, g = slab // groups, slab % groups
    lines = levels_of(power_ref[: 2 * (sources // groups)] * depth, sizes_ref[...], scales_ref[...], cells)
    half_lines = len(lines) // 2
    own, mirror = lines[0], lines[half_lines]
    for other in range(1, half_lines):
        own = jnp.where(h == other, lines[other], own)
        mirror = jnp.where(h == other, lines[half_lines + other], mirror)
    lane = lax.broadcasted_iota(jnp.int32, (1, LANES), 1)
    edge = (lane == 0) & (h == 0)
    level_zero, level_mid = lines[0], lines[half_lines]
    upper = g >= groups // 2
    edge_level = jnp.where(upper, level_mid, level_zero)
    one = jnp.where(edge, edge_level, own)
    two = jnp.where(edge, edge_level, mirror)
    packed_here = (shot == 0) & (h == 0) & ((g == 0) | (g == groups // 2))
    packed = (lane == 0) & packed_here
    pieces = []
    for c in range(2):
        for r in range(rows):
            start = (c * rows + r) * planes
            pieces.append(in_ref[:, start : start + planes, :].reshape(depth, LANES))
    value = split(jnp.concatenate(pieces, axis=1))
    table = (zh_ref[...], zl_ref[...])
    both = dot3(table, value)
    shrunk_r, shrunk_i = [], []
    for r in range(rows):
        real = slice(r * LANES, (r + 1) * LANES)
        imag = slice((rows + r) * LANES, (rows + r + 1) * LANES)
        cr, sr = both[:depth, real], both[depth:, real]
        ci, si = both[:depth, imag], both[depth:, imag]
        zr, zi = cr + si, ci - sr
        energy = zr * zr + zi * zi
        if r == 0:
            energy_a = jnp.where(packed, cr * cr + sr * sr, energy)
            energy_b = jnp.where(packed, ci * ci + si * si, energy)
            one_a = jnp.where(packed, level_zero, one)
            two_a = jnp.where(packed, level_zero, two)
            one_b = jnp.where(packed, level_mid, one)
            two_b = jnp.where(packed, level_mid, two)
            factor_a = mean_factor(energy_a, one_a, two_a)
            factor_b = mean_factor(energy_b, one_b, two_b)
            shrunk_r.append(factor_a * cr + factor_b * si)
            shrunk_i.append(factor_b * ci - factor_a * sr)
        else:
            factor = mean_factor(energy, one, two)
            shrunk_r.append(factor * zr)
            shrunk_i.append(factor * zi)
    back = dot3(table, split(jnp.concatenate(shrunk_r + shrunk_i, axis=1)))
    wide = rows * LANES
    out_ref[:, 0, :wide] = back[:depth, :wide] - back[depth:, wide:]
    out_ref[:, 0, wide:] = back[:depth, wide:] + back[depth:, :wide]


def mean_factor(energy, one, two):
    magnitude = jnp.sqrt(energy)
    first = jnp.maximum(magnitude - one, 0.0) / jnp.maximum(magnitude, one)
    second = jnp.maximum(magnitude - two, 0.0) / jnp.maximum(magnitude, two)
    return 0.5 * (first + second)


def shrink(place, received, power, sizes, scales, tables, groups, cells):
    zh, zl = tables
    depth = zh.shape[1]
    planes = depth // received.shape[0]
    wide = (received.shape[1] - 8) // planes * LANES
    vmem = pl.BlockSpec(memory_space=pltpu.VMEM)
    return pl.pallas_call(
        functools.partial(shrink_kernel, groups, float(cells)),
        in_specs=[pl.BlockSpec(memory_space=pltpu.SMEM)] + [vmem] * 6,
        out_specs=vmem,
        out_shape=jax.ShapeDtypeStruct((depth, 1, wide), F32),
        compiler_params=ROOM,
        name="shrink",
        interpret=INTERPRET,
    )(place, received, power, sizes, scales, zh, zl)


def image_kernel(groups, scale, in_ref, bh_ref, bl_ref, xh_ref, xl_ref, out_ref):
    count, _, wide = in_ref.shape
    rows = wide // (2 * LANES)
    halves_x = xh_ref.shape[0]
    per_half = count // halves_x
    mid = per_half // 2
    row = lax.broadcasted_iota(jnp.int32, (mid, LANES), 0)
    lane = lax.broadcasted_iota(jnp.int32, (mid, LANES), 1)
    columns = [[], []]
    for h in range(halves_x):
        cos_r, cos_i, sin_r, sin_i = [], [], [], []
        for r in range(rows):
            real = slice(r * LANES, (r + 1) * LANES)
            imag = slice((rows + r) * LANES, (rows + r + 1) * LANES)
            low = slice(h * per_half, h * per_half + mid)
            high = slice(h * per_half + mid, (h + 1) * per_half)
            pr, pi = in_ref[low, 0, real], in_ref[low, 0, imag]
            nr, ni = in_ref[high, 0, real], in_ref[high, 0, imag]
            cr, ci, sr, si = pr + nr, pi + ni, ni - pi, pr - nr
            if h == 0:
                lane0 = lane == 0
                cr = jnp.where(lane0, 2.0 * pr, cr)
                ci = jnp.where(lane0, 2.0 * nr, ci)
                sr = jnp.where(lane0, -2.0 * pi, sr)
                si = jnp.where(lane0, -2.0 * ni, si)
            if r == 0:
                row0 = row == 0
                cr = jnp.where(row0, pr, cr)
                ci = jnp.where(row0, pi, ci)
                sr = jnp.where(row0, nr, sr)
                si = jnp.where(row0, ni, si)
            cos_r.append(cr)
            cos_i.append(ci)
            sin_r.append(sr)
            sin_i.append(si)
        columns[0].append(jnp.concatenate(cos_r + sin_r, axis=0))
        columns[1].append(jnp.concatenate(cos_i + sin_i, axis=0))
    stacked = jnp.concatenate(columns[0] + columns[1], axis=1)
    along_y = dot3((bh_ref[...], bl_ref[...]), split(stacked))
    lanes = lax.broadcasted_iota(jnp.int32, (1, along_y.shape[1]), 1)
    single = (lanes == 0) | (lanes == along_y.shape[1] // 2)
    along_y = along_y * jnp.where(single, scale, 2.0 * scale)
    high, low = split(along_y)
    half = along_y.shape[1] // 2
    parts = []
    for h in range(halves_x):
        own = slice(h * LANES, (h + 1) * LANES)
        other = slice(half + h * LANES, half + (h + 1) * LANES)
        value = [jnp.concatenate([a[:, own], a[:, other]], axis=1) for a in (high, low)]
        parts.append(dot3(value, (xh_ref[h], xl_ref[h]), (((1,), (1,)), ((), ()))))
    out_ref[0, :, :half] = parts[0] + parts[1]
    out_ref[0, :, half:] = parts[0] - parts[1]


def image_of(returned, back_tables, x_tables, groups, scale, shape):
    vmem = pl.BlockSpec(memory_space=pltpu.VMEM)
    return pl.pallas_call(
        functools.partial(image_kernel, groups, scale),
        in_specs=[vmem] * 5,
        out_specs=vmem,
        out_shape=jax.ShapeDtypeStruct(shape, F32),
        compiler_params=ROOM,
        name="image",
        interpret=INTERPRET,
    )(returned, *back_tables, *x_tables)


def on_device(source_field, receiver_fields, weights, model, wedge_sizes, wedge_scales):
    planes, width_y, width_x = source_field.shape[1:]
    shots = lax.axis_size("shot")
    slabs = lax.axis_size(SLAB)
    depth = planes * slabs
    groups = slabs // (width_x // 2 // LANES)
    rows = width_y // shots // groups
    shot = lax.axis_index("shot").astype(jnp.int32)
    slab = lax.axis_index(SLAB).astype(jnp.int32)
    x_tables = halves(x_table(width_x))
    y_tables = halves(y_table(width_y))
    z_tables = halves(z_table(depth))
    back_tables = halves(y_back_table(width_y, shots, groups // 2, rows))
    chunk = planes // CHUNKS
    came, rests = [], []
    for q in range(CHUNKS):
        way = 1 - 2 * (q % 2)
        start, rest = plane_terms(
            weights, shot[None], source_field, receiver_fields, model, x_tables + y_tables,
            shots, q * chunk, chunk, way,
        )
        came.append(start)
        rests.append(rest)
    for step in range(shots - 1):
        for q in range(CHUNKS):
            way = 1 - 2 * (q % 2)
            moved = lax.ppermute(came[q], "shot", [(i, (i + way) % shots) for i in range(shots)])
            came[q] = moved if step == shots - 2 else moved + rests[q][step]
    message = pack(shot[None], came, rests, groups)
    received = lax.all_to_all(message, SLAB, split_axis=0, concat_axis=0, tiled=True)
    base = 2 * rows * planes
    power = jnp.sum(received[:, base:, :], axis=0)
    power = jnp.broadcast_to(power[None], (shots,) + power.shape)
    power = jnp.sum(lax.all_to_all(power, "shot", split_axis=0, concat_axis=0, tiled=True), axis=0)
    shrunk = shrink(
        jnp.stack([shot, slab]),
        received,
        power,
        wedge_sizes[None],
        wedge_scales[None],
        z_tables,
        groups,
        depth * width_y,
    )
    returned = lax.all_to_all(shrunk, SLAB_SHOT, split_axis=0, concat_axis=0, tiled=True)
    scale = 1.0 / (depth * width_y * width_x)
    return image_of(returned, back_tables, x_tables, groups, scale, model.shape)


def solution(mesh):
    torus = Mesh(
        mesh.devices.reshape(mesh.shape["shot"], 4, 4, 2), ("shot", "slab_0", "slab_1", "slab_2")
    )
    return jax.shard_map(
        on_device,
        mesh=torus,
        in_specs=(
            P("shot", SLAB, None, None),
            P("shot", SLAB, None, None),
            P("shot"),
            P(SLAB_SHOT, None, None),
            P(),
            P(),
        ),
        out_specs=P(SLAB_SHOT, None, None),
        check_vma=False,
    )
```

```python
import functools

import jax
import jax.numpy as jnp
import numpy as np
from jax import lax
from jax.experimental import pallas as pl
from jax.experimental.pallas import tpu as pltpu
from jax.sharding import Mesh
from jax.sharding import PartitionSpec as P

SLAB = ("slab_0", "slab_1", "slab_2")
SLAB_SHOT = ("slab_0", "slab_1", "slab_2", "shot")

STEP_SIZE = 0.25
EPSILON = 1e-06
LANES = 128
F32 = jnp.float32
BF16 = jnp.bfloat16
INTERPRET = False
CHUNKS = 4
ROOM = pltpu.CompilerParams(vmem_limit_bytes=24 * 1024 * 1024)


def halves(table):
    high = np.asarray(table, dtype=np.float32).astype(jnp.bfloat16)
    low = (np.asarray(table) - high.astype(np.float64)).astype(np.float32).astype(jnp.bfloat16)
    return jnp.asarray(high), jnp.asarray(low)


def angles(rows, columns, length):
    return 2.0 * np.pi * (np.outer(rows, columns) % length) / length


def x_table(width):
    half = width // 2
    tables = []
    for h in range(2):
        angle = angles(np.arange(half), np.arange(h, half, 2), width)
        sine = -np.sin(angle)
        if h == 0:
            sine[:, 0] = 1.0 - 2.0 * (np.arange(half) % 2)
        tables.append(np.concatenate([np.cos(angle), sine], axis=1))
    return np.stack(tables)


def y_order(width):
    half = width // 2
    return np.concatenate([np.arange(0, half, 2), np.arange(1, half, 2)])


def y_rows(width, length):
    angle = angles(y_order(width), np.arange(length), width)
    sine = np.sin(angle)
    sine[0] = 1.0 - 2.0 * (np.arange(length) % 2)
    return np.cos(angle), sine


def y_table(width):
    cos, sin = y_rows(width, width // 2)
    quarter = width // 4
    return np.stack(
        [np.concatenate([cos[part], sin[part]]) for part in (slice(0, quarter), slice(quarter, None))]
    )


def y_back_table(width, shots, parts, rows):
    half = width // 2
    r, g, j = np.meshgrid(np.arange(rows), np.arange(parts), np.arange(shots), indexing="ij")
    slot = (j * (half // shots) + g * rows + r).reshape(-1)
    cos, sin = y_rows(width, width)
    return np.concatenate([cos[slot].T, sin[slot].T], axis=1)


def z_table(depth):
    angle = angles(np.arange(depth), np.arange(depth), depth)
    return np.concatenate([np.cos(angle), np.sin(angle)], axis=0)


def split(value):
    high = value.astype(BF16)
    low = (value - high.astype(F32)).astype(BF16)
    return high, low


def dot(a, b, dims=(((1,), (0,)), ((), ()))):
    return lax.dot_general(a, b, dims, preferred_element_type=F32)


def dot3(a, b, dims=(((1,), (0,)), ((), ()))):
    return dot(a[0], b[0], dims) + (dot(a[1], b[0], dims) + dot(a[0], b[1], dims))


def plane_kernel(
    shots, first, weight_ref, shot_ref, source_ref, receiver_ref, model_ref, xh_ref, xl_ref, yh_ref, yl_ref,
    up_ref, down_ref, rest_ref, keep_ref
):
    step = pl.program_id(0)
    plane = step + first
    per_way = pl.num_programs(0) // 2
    way = jnp.where(step < per_way, 1, -1)
    members = receiver_ref.shape[0]
    own = (plane == shot_ref[0]).astype(F32)
    width_y, width_x = source_ref.shape[2:]
    rows, half = width_y // 2, width_x // 2
    encoded = weight_ref[0].astype(F32) * receiver_ref[0, 0].astype(F32)
    for member in range(1, members):
        encoded = encoded + weight_ref[member].astype(F32) * receiver_ref[member, 0].astype(F32)
    term = source_ref[0, 0].astype(F32) * encoded
    term = own * model_ref[0].astype(F32) - STEP_SIZE * term
    low, high = term[:, :half], term[:, half:]
    cosines, sines = [], []
    for h, fold in ((0, low + high), (1, low - high)):
        fold = jnp.concatenate([fold[:rows] + fold[rows:], fold[:rows] - fold[rows:]], axis=0)
        along_x = dot3(split(fold), (xh_ref[h], xl_ref[h]))
        cosines.append(along_x[:, : half // 2])
        sines.append(along_x[:, half // 2 :])
    along_x = jnp.concatenate(cosines + sines, axis=1)
    quarter = rows // 2
    row = lax.broadcasted_iota(jnp.int32, (quarter, half), 0)
    lane0 = lax.broadcasted_iota(jnp.int32, (quarter, half), 1) == 0
    for parity in range(2):
        both = dot3((yh_ref[parity], yl_ref[parity]), split(along_x[parity * rows : (parity + 1) * rows]))
        cr, ci = both[:quarter, :half], both[:quarter, half:]
        sr, si = both[quarter:, :half], both[quarter:, half:]
        part = pl.ds(parity * quarter, quarter)
        if parity == 0:
            row0 = row == 0
            keep_ref[0, part] = jnp.where(row0 | lane0, cr, cr + si)
            keep_ref[1, part] = jnp.where(row0, ci, jnp.where(lane0, -sr, ci - sr))
            keep_ref[2, part] = jnp.where(row0, sr, jnp.where(lane0, ci, cr - si))
            keep_ref[3, part] = jnp.where(row0, si, jnp.where(lane0, -si, ci + sr))
        else:
            keep_ref[0, part] = jnp.where(lane0, cr, cr + si)
            keep_ref[1, part] = jnp.where(lane0, -sr, ci - sr)
            keep_ref[2, part] = jnp.where(lane0, ci, cr - si)
            keep_ref[3, part] = jnp.where(lane0, -si, ci + sr)
    block = rows // shots

    def give(order, target):
        owner = lax.rem(shot_ref[0] + 2 * shots - way * (1 + order), shots)
        part = pl.ds(pl.multiple_of(owner * block, 8), block)
        target[0, :block] = keep_ref[0, part]
        target[1, :block] = keep_ref[1, part]
        target[0, block:] = keep_ref[2, part]
        target[1, block:] = keep_ref[3, part]

    @pl.when(step < per_way)
    def _():
        give(0, up_ref.at[0])

    @pl.when(step >= per_way)
    def _():
        give(0, down_ref.at[0])

    for order in range(1, shots):
        give(order, rest_ref.at[order - 1, 0])


def plane_terms(weights, shot, source, receivers, model, tables, shots, first, count):
    _, planes, width_y, width_x = source.shape
    members = receivers.shape[0]
    xh, xl, yh, yl = tables
    whole = lambda a: pl.BlockSpec(a.shape, lambda p: (0,) * a.ndim)
    piece = (2, width_y // shots, width_x // 2)
    return pl.pallas_call(
        functools.partial(plane_kernel, shots, first),
        grid=(count,),
        in_specs=[
            pl.BlockSpec(memory_space=pltpu.SMEM),
            pl.BlockSpec(memory_space=pltpu.SMEM),
            pl.BlockSpec((1, 1, width_y, width_x), lambda p: (0, p + first, 0, 0)),
            pl.BlockSpec((members, 1, width_y, width_x), lambda p: (0, p + first, 0, 0)),
            whole(model),
            whole(xh),
            whole(xl),
            whole(yh),
            whole(yl),
        ],
        out_specs=[
            pl.BlockSpec((1,) + piece, lambda p: (jnp.minimum(p, count // 2 - 1), 0, 0, 0)),
            pl.BlockSpec((1,) + piece, lambda p: (jnp.maximum(p - count // 2, 0), 0, 0, 0)),
            pl.BlockSpec((shots - 1, 1) + piece, lambda p: (0, p, 0, 0, 0)),
        ],
        out_shape=[
            jax.ShapeDtypeStruct((count // 2,) + piece, F32),
            jax.ShapeDtypeStruct((count // 2,) + piece, F32),
            jax.ShapeDtypeStruct((shots - 1, count) + piece, F32),
        ],
        scratch_shapes=[pltpu.VMEM((4, width_y // 2, width_x // 2), F32)],
        cost_estimate=pl.CostEstimate(
            flops=count * 3 * width_y * width_x * (width_x + width_y),
            bytes_accessed=count * 10 * width_y * width_x,
            transcendentals=0,
        ),
        name="plane_terms",
        interpret=INTERPRET,
    )(weights, shot, source, receivers, model, xh, xl, yh, yl)


def pack_kernel(groups, chunks, shot_ref, *refs):
    ins, out_ref = refs[:-1], refs[-1]
    planes = sum(ref.shape[0] for ref in ins[:chunks])
    own = []
    for last in ins[chunks:]:
        middle = last.shape[1] // 2
        own += [(last, slice(0, middle)), (last, slice(middle, None))]
    _, _, slots, half = ins[0].shape
    rows = slots // groups
    halves_x = half // LANES
    first = shot_ref[0] == 0
    lane0 = lax.broadcasted_iota(jnp.int32, (1, LANES), 1) == 0

    def plane_lines(c, slot, h):
        lanes = slice(h * LANES, (h + 1) * LANES)
        parts = [
            came[:, c, slot, lanes] + last[0, part, c, slot, lanes]
            for came, (last, part) in zip(ins[:chunks], own)
        ]
        return jnp.concatenate(parts, axis=0)

    pos = [jnp.zeros((planes, LANES), F32) for _ in range(halves_x)]
    neg = [jnp.zeros((planes, LANES), F32) for _ in range(halves_x)]
    fix_a = jnp.zeros((planes, LANES), F32)
    fix_b = jnp.zeros((planes, LANES), F32)
    for slot in range(slots):
        g, r = divmod(slot, rows)
        for h in range(halves_x):
            real = plane_lines(0, slot, h)
            imag = plane_lines(1, slot, h)
            d = h * groups + g
            out_ref[d, r * planes : (r + 1) * planes] = real
            out_ref[d, (rows + r) * planes : (rows + r + 1) * planes] = imag
            real2, imag2 = real * real, imag * imag
            energy = real2 + imag2
            if h == 0 and slot in (0, slots // 2):
                fix_a = fix_a + real2
                fix_b = fix_b + imag2
                special = lane0 & first
                energy = jnp.where(special, 0.0, energy)
            if slot < slots // 2:
                pos[h] = pos[h] + energy
            else:
                neg[h] = neg[h] + energy
    keep = first.astype(F32)
    lines = []
    for side, fix in ((pos, fix_a), (neg, fix_b)):
        for h in range(halves_x):
            total = pos[h] + neg[h]
            lines.append(jnp.where(lane0, 2.0 * side[0] + keep * fix, total) if h == 0 else total)
    sums = jnp.concatenate([jnp.sum(line, axis=0, keepdims=True) for line in lines], axis=0)
    sums = jnp.concatenate([sums, jnp.zeros((8 - sums.shape[0], LANES), F32)], axis=0)
    base = 2 * rows * planes
    for d in range(halves_x * groups):
        out_ref[d, base : base + 8] = sums


def pack(shot, came, rests, groups):
    chunks = len(came)
    planes = sum(a.shape[0] for a in came)
    _, _, slots, half = came[0].shape
    rows = slots // groups
    out_shape = (groups * (half // LANES), 2 * rows * planes + 8, LANES)
    return pl.pallas_call(
        functools.partial(pack_kernel, groups, chunks),
        grid=(1,),
        in_specs=[pl.BlockSpec(memory_space=pltpu.SMEM)]
        + [pl.BlockSpec(a.shape, lambda i: (0, 0, 0, 0)) for a in came]
        + [pl.BlockSpec((1,) + a.shape[1:], lambda i, last=a.shape[0] - 1: (last, 0, 0, 0, 0)) for a in rests],
        out_specs=pl.BlockSpec(out_shape, lambda i: (0, 0, 0)),
        out_shape=jax.ShapeDtypeStruct(out_shape, F32),
        cost_estimate=pl.CostEstimate(flops=10**9, bytes_accessed=10**6, transcendentals=0),
        compiler_params=ROOM,
        name="pack",
        interpret=INTERPRET,
    )(shot, *came, *rests)


def levels_of(power, sizes, scales, cells):
    wedges = sizes.shape[1]
    down = lax.broadcasted_iota(jnp.int32, (wedges, wedges), 0)
    across = lax.broadcasted_iota(jnp.int32, (wedges, wedges), 1)
    size_row = jnp.broadcast_to(sizes.astype(F32), (wedges, wedges))
    scale_row = jnp.broadcast_to(scales, (wedges, wedges))
    ends = jnp.sum(jnp.where(across <= down, size_row, 0.0), axis=1, keepdims=True)
    size = jnp.sum(jnp.where(across == down, size_row, 0.0), axis=1, keepdims=True)
    scale = jnp.sum(jnp.where(across == down, scale_row, 0.0), axis=1, keepdims=True)
    starts = ends - size
    half_lines = power.shape[0] // 2
    half = half_lines * LANES
    members = []
    total = jnp.zeros((wedges, 1), F32)
    for line in range(2 * half_lines):
        column = half_lines * lax.broadcasted_iota(jnp.int32, (wedges, LANES), 1) + line % half_lines
        if line >= half_lines:
            column = jnp.where(column == 0, half, 2 * half - column)
        column = column.astype(F32)
        member = (column >= starts) & (column < ends)
        members.append(member)
        total = total + jnp.sum(jnp.where(member, power[line : line + 1], 0.0), axis=1, keepdims=True)
    spread = jnp.sqrt(total / (size * cells) + EPSILON)
    level = scale * spread
    return [jnp.sum(jnp.where(member, level, 0.0), axis=0, keepdims=True) for member in members]


def depth_kernel(in_ref, zh_ref, zl_ref, out_ref):
    sources, message, _ = in_ref.shape
    depth = zh_ref.shape[1]
    planes = depth // sources
    pieces = []
    for start in range(0, message - 8, planes):
        pieces.append(in_ref[:, start : start + planes, :].reshape(depth, LANES))
    out_ref[...] = dot3((zh_ref[...], zl_ref[...]), split(jnp.concatenate(pieces, axis=1)))


def along_depth(received, tables):
    vmem = pl.BlockSpec(memory_space=pltpu.VMEM)
    zh, zl = tables
    planes = zh.shape[1] // received.shape[0]
    wide = (received.shape[1] - 8) // planes * LANES
    return pl.pallas_call(
        depth_kernel,
        in_specs=[vmem] * 3,
        out_specs=vmem,
        out_shape=jax.ShapeDtypeStruct((zh.shape[0], wide), F32),
        cost_estimate=pl.CostEstimate(flops=4 * 10**9, bytes_accessed=3 * 10**6, transcendentals=0),
        compiler_params=ROOM,
        name="along_depth",
        interpret=INTERPRET,
    )(received, zh, zl)


def shrink_kernel(
    groups, slabs, cells, place_ref, both_ref, power_ref, sizes_ref, scales_ref, zh_ref, zl_ref, out_ref
):
    depth = zh_ref.shape[1]
    rows = both_ref.shape[1] // (2 * LANES)
    shot, slab = place_ref[0], place_ref[1]
    h, g = slab // groups, slab % groups
    lines = levels_of(power_ref[: 2 * (slabs // groups)] * depth, sizes_ref[...], scales_ref[...], cells)
    half_lines = len(lines) // 2
    own, mirror = lines[0], lines[half_lines]
    for other in range(1, half_lines):
        own = jnp.where(h == other, lines[other], own)
        mirror = jnp.where(h == other, lines[half_lines + other], mirror)
    lane = lax.broadcasted_iota(jnp.int32, (1, LANES), 1)
    edge = (lane == 0) & (h == 0)
    level_zero, level_mid = lines[0], lines[half_lines]
    upper = g >= groups // 2
    edge_level = jnp.where(upper, level_mid, level_zero)
    one = jnp.where(edge, edge_level, own)
    two = jnp.where(edge, edge_level, mirror)
    packed_here = (shot == 0) & (h == 0) & ((g == 0) | (g == groups // 2))
    packed = (lane == 0) & packed_here
    table = (zh_ref[...], zl_ref[...])
    shrunk_r, shrunk_i = [], []
    for r in range(rows):
        real = slice(r * LANES, (r + 1) * LANES)
        imag = slice((rows + r) * LANES, (rows + r + 1) * LANES)
        cr, sr = both_ref[:depth, real], both_ref[depth:, real]
        ci, si = both_ref[:depth, imag], both_ref[depth:, imag]
        zr, zi = cr + si, ci - sr
        energy = zr * zr + zi * zi
        if r == 0:
            energy_a = jnp.where(packed, cr * cr + sr * sr, energy)
            energy_b = jnp.where(packed, ci * ci + si * si, energy)
            one_a = jnp.where(packed, level_zero, one)
            two_a = jnp.where(packed, level_zero, two)
            one_b = jnp.where(packed, level_mid, one)
            two_b = jnp.where(packed, level_mid, two)
            factor_a = mean_factor(energy_a, one_a, two_a)
            factor_b = mean_factor(energy_b, one_b, two_b)
            shrunk_r.append(factor_a * cr + factor_b * si)
            shrunk_i.append(factor_b * ci - factor_a * sr)
        else:
            factor = mean_factor(energy, one, two)
            shrunk_r.append(factor * zr)
            shrunk_i.append(factor * zi)
    back = dot3(table, split(jnp.concatenate(shrunk_r + shrunk_i, axis=1)))
    wide = rows * LANES
    out_ref[:, 0, :wide] = back[:depth, :wide] - back[depth:, wide:]
    out_ref[:, 0, wide:] = back[:depth, wide:] + back[depth:, :wide]


def mean_factor(energy, one, two):
    magnitude = jnp.sqrt(energy)
    first = jnp.maximum(magnitude - one, 0.0) / jnp.maximum(magnitude, one)
    second = jnp.maximum(magnitude - two, 0.0) / jnp.maximum(magnitude, two)
    return 0.5 * (first + second)


def shrink(place, both, power, sizes, scales, tables, groups, slabs, cells):
    zh, zl = tables
    depth, wide = zh.shape[1], both.shape[1]
    vmem = pl.BlockSpec(memory_space=pltpu.VMEM)
    return pl.pallas_call(
        functools.partial(shrink_kernel, groups, slabs, float(cells)),
        in_specs=[pl.BlockSpec(memory_space=pltpu.SMEM)] + [vmem] * 6,
        out_specs=vmem,
        out_shape=jax.ShapeDtypeStruct((depth, 1, wide), F32),
        compiler_params=ROOM,
        name="shrink",
        interpret=INTERPRET,
    )(place, both, power, sizes, scales, zh, zl)


def image_kernel(groups, scale, in_ref, bh_ref, bl_ref, xh_ref, xl_ref, out_ref):
    count, _, wide = in_ref.shape
    rows = wide // (2 * LANES)
    halves_x = xh_ref.shape[0]
    per_half = count // halves_x
    mid = per_half // 2
    row = lax.broadcasted_iota(jnp.int32, (mid, LANES), 0)
    lane = lax.broadcasted_iota(jnp.int32, (mid, LANES), 1)
    columns = [[], []]
    for h in range(halves_x):
        cos_r, cos_i, sin_r, sin_i = [], [], [], []
        for r in range(rows):
            real = slice(r * LANES, (r + 1) * LANES)
            imag = slice((rows + r) * LANES, (rows + r + 1) * LANES)
            low = slice(h * per_half, h * per_half + mid)
            high = slice(h * per_half + mid, (h + 1) * per_half)
            pr, pi = in_ref[low, 0, real], in_ref[low, 0, imag]
            nr, ni = in_ref[high, 0, real], in_ref[high, 0, imag]
            cr, ci, sr, si = pr + nr, pi + ni, ni - pi, pr - nr
            if h == 0:
                lane0 = lane == 0
                cr = jnp.where(lane0, 2.0 * pr, cr)
                ci = jnp.where(lane0, 2.0 * nr, ci)
                sr = jnp.where(lane0, -2.0 * pi, sr)
                si = jnp.where(lane0, -2.0 * ni, si)
            if r == 0:
                row0 = row == 0
                cr = jnp.where(row0, pr, cr)
                ci = jnp.where(row0, pi, ci)
                sr = jnp.where(row0, nr, sr)
                si = jnp.where(row0, ni, si)
            cos_r.append(cr)
            cos_i.append(ci)
            sin_r.append(sr)
            sin_i.append(si)
        columns[0].append(jnp.concatenate(cos_r + sin_r, axis=0))
        columns[1].append(jnp.concatenate(cos_i + sin_i, axis=0))
    stacked = jnp.concatenate(columns[0] + columns[1], axis=1)
    along_y = dot3((bh_ref[...], bl_ref[...]), split(stacked))
    lanes = lax.broadcasted_iota(jnp.int32, (1, along_y.shape[1]), 1)
    single = (lanes == 0) | (lanes == along_y.shape[1] // 2)
    along_y = along_y * jnp.where(single, scale, 2.0 * scale)
    high, low = split(along_y)
    half = along_y.shape[1] // 2
    parts = []
    for h in range(halves_x):
        own = slice(h * LANES, (h + 1) * LANES)
        other = slice(half + h * LANES, half + (h + 1) * LANES)
        value = [jnp.concatenate([a[:, own], a[:, other]], axis=1) for a in (high, low)]
        parts.append(dot3(value, (xh_ref[h], xl_ref[h]), (((1,), (1,)), ((), ()))))
    out_ref[0, :, :half] = parts[0] + parts[1]
    out_ref[0, :, half:] = parts[0] - parts[1]


def image_of(returned, back_tables, x_tables, groups, scale, shape):
    vmem = pl.BlockSpec(memory_space=pltpu.VMEM)
    return pl.pallas_call(
        functools.partial(image_kernel, groups, scale),
        in_specs=[vmem] * 5,
        out_specs=vmem,
        out_shape=jax.ShapeDtypeStruct(shape, F32),
        compiler_params=ROOM,
        name="image",
        interpret=INTERPRET,
    )(returned, *back_tables, *x_tables)


def on_device(source_field, receiver_fields, weights, model, wedge_sizes, wedge_scales):
    planes, width_y, width_x = source_field.shape[1:]
    shots = lax.axis_size("shot")
    slabs = lax.axis_size(SLAB)
    depth = planes * slabs
    groups = slabs // (width_x // 2 // LANES)
    rows = width_y // shots // groups
    shot = lax.axis_index("shot").astype(jnp.int32)
    slab = lax.axis_index(SLAB).astype(jnp.int32)
    x_tables = halves(x_table(width_x))
    y_tables = halves(y_table(width_y))
    z_tables = halves(z_table(depth))
    back_tables = halves(y_back_table(width_y, shots, groups // 2, rows))
    chunk = planes // (CHUNKS // 2)
    came, rests = [], []
    for q in range(CHUNKS // 2):
        up, down, rest = plane_terms(
            weights, shot[None], source_field, receiver_fields, model, x_tables + y_tables, shots, q * chunk, chunk
        )
        came += [up, down]
        rests.append(rest)
    half = chunk // 2
    for step in range(shots - 1):
        for q in range(CHUNKS):
            way = 1 - 2 * (q % 2)
            moved = lax.ppermute(came[q], "shot", [(i, (i + way) % shots) for i in range(shots)])
            if step < shots - 2:
                moved = moved + rests[q // 2][step, (q % 2) * half : (q % 2 + 1) * half]
            came[q] = moved
    message = pack(shot[None], came, rests, groups)
    received = lax.all_to_all(message, SLAB, split_axis=0, concat_axis=0, tiled=True)
    base = 2 * rows * planes
    power = jnp.sum(received[:, base:, :], axis=0)
    power = jnp.broadcast_to(power[None], (shots,) + power.shape)
    power = jnp.sum(lax.all_to_all(power, "shot", split_axis=0, concat_axis=0, tiled=True), axis=0)
    shrunk = shrink(
        jnp.stack([shot, slab]),
        along_depth(received, z_tables),
        power,
        wedge_sizes[None],
        wedge_scales[None],
        z_tables,
        groups,
        slabs,
        depth * width_y,
    )
    returned = lax.all_to_all(shrunk, SLAB_SHOT, split_axis=0, concat_axis=0, tiled=True)
    scale = 1.0 / (depth * width_y * width_x)
    return image_of(returned, back_tables, x_tables, groups, scale, model.shape)


def solution(mesh):
    torus = Mesh(
        mesh.devices.reshape(mesh.shape["shot"], 4, 4, 2), ("shot", "slab_0", "slab_1", "slab_2")
    )
    return jax.shard_map(
        on_device,
        mesh=torus,
        in_specs=(
            P("shot", SLAB, None, None),
            P("shot", SLAB, None, None),
            P("shot"),
            P(SLAB_SHOT, None, None),
            P(),
            P(),
        ),
        out_specs=P(SLAB_SHOT, None, None),
        check_vma=False,
    )
```

```python
import functools

import jax
import jax.numpy as jnp
import numpy as np
from jax import lax
from jax.experimental import pallas as pl
from jax.experimental.pallas import tpu as pltpu
from jax.sharding import Mesh
from jax.sharding import PartitionSpec as P

SLAB = ("slab_0", "slab_1", "slab_2")
SLAB_SHOT = ("slab_0", "slab_1", "slab_2", "shot")

STEP_SIZE = 0.25
EPSILON = 1e-06
LANES = 128
F32 = jnp.float32
BF16 = jnp.bfloat16
INTERPRET = False
CHUNKS = 4
ROOM = pltpu.CompilerParams(vmem_limit_bytes=24 * 1024 * 1024)


def halves(table):
    high = np.asarray(table, dtype=np.float32).astype(jnp.bfloat16)
    low = (np.asarray(table) - high.astype(np.float64)).astype(np.float32).astype(jnp.bfloat16)
    return jnp.asarray(np.stack([high, low]))


def angles(rows, columns, length):
    return 2.0 * np.pi * (np.outer(rows, columns) % length) / length


def x_table(width):
    half = width // 2
    tables = []
    for h in range(2):
        angle = angles(np.arange(half), np.arange(h, half, 2), width)
        sine = -np.sin(angle)
        if h == 0:
            sine[:, 0] = 1.0 - 2.0 * (np.arange(half) % 2)
        tables.append(np.concatenate([np.cos(angle), sine], axis=1))
    return np.stack(tables)


def y_order(width):
    half = width // 2
    return np.concatenate([np.arange(0, half, 2), np.arange(1, half, 2)])


def y_rows(width, length):
    angle = angles(y_order(width), np.arange(length), width)
    sine = np.sin(angle)
    sine[0] = 1.0 - 2.0 * (np.arange(length) % 2)
    return np.cos(angle), sine


def y_table(width):
    cos, sin = y_rows(width, width // 2)
    quarter = width // 4
    return np.stack(
        [np.concatenate([cos[part], sin[part]]) for part in (slice(0, quarter), slice(quarter, None))]
    )


def y_back_table(width, shots, parts, rows):
    half = width // 2
    r, g, j = np.meshgrid(np.arange(rows), np.arange(parts), np.arange(shots), indexing="ij")
    slot = (j * (half // shots) + g * rows + r).reshape(-1)
    cos, sin = y_rows(width, width)
    return np.concatenate([cos[slot].T, sin[slot].T], axis=1)


def z_table(depth):
    angle = angles(np.arange(depth), np.arange(depth), depth)
    return np.concatenate([np.cos(angle), np.sin(angle)], axis=0)


def split(value):
    high = value.astype(BF16)
    low = (value - high.astype(F32)).astype(BF16)
    return high, low


def dot(a, b, dims=(((1,), (0,)), ((), ()))):
    return lax.dot_general(a, b, dims, preferred_element_type=F32)


def dot3(a, b, dims=(((1,), (0,)), ((), ()))):
    return dot(a[0], b[0], dims) + (dot(a[1], b[0], dims) + dot(a[0], b[1], dims))


def plane_kernel(
    shots, first, weight_ref, shot_ref, source_ref, receiver_ref, model_ref, x_ref, y_ref,
    up_ref, down_ref, rest_ref, keep_ref
):
    step = pl.program_id(0)
    plane = step + first
    per_way = pl.num_programs(0) // 2
    way = jnp.where(step < per_way, 1, -1)
    members = receiver_ref.shape[0]
    own = (plane == shot_ref[0]).astype(F32)
    width_y, width_x = source_ref.shape[2:]
    rows, half = width_y // 2, width_x // 2
    encoded = weight_ref[0].astype(F32) * receiver_ref[0, 0].astype(F32)
    for member in range(1, members):
        encoded = encoded + weight_ref[member].astype(F32) * receiver_ref[member, 0].astype(F32)
    term = source_ref[0, 0].astype(F32) * encoded
    term = own * model_ref[0].astype(F32) - STEP_SIZE * term
    low, high = term[:, :half], term[:, half:]
    cosines, sines = [], []
    for h, fold in ((0, low + high), (1, low - high)):
        fold = jnp.concatenate([fold[:rows] + fold[rows:], fold[:rows] - fold[rows:]], axis=0)
        along_x = dot3(split(fold), (x_ref[0, h], x_ref[1, h]))
        cosines.append(along_x[:, : half // 2])
        sines.append(along_x[:, half // 2 :])
    along_x = jnp.concatenate(cosines + sines, axis=1)
    quarter = rows // 2
    row = lax.broadcasted_iota(jnp.int32, (quarter, half), 0)
    lane0 = lax.broadcasted_iota(jnp.int32, (quarter, half), 1) == 0
    for parity in range(2):
        both = dot3((y_ref[0, parity], y_ref[1, parity]), split(along_x[parity * rows : (parity + 1) * rows]))
        cr, ci = both[:quarter, :half], both[:quarter, half:]
        sr, si = both[quarter:, :half], both[quarter:, half:]
        part = pl.ds(parity * quarter, quarter)
        if parity == 0:
            row0 = row == 0
            keep_ref[0, part] = jnp.where(row0 | lane0, cr, cr + si)
            keep_ref[1, part] = jnp.where(row0, ci, jnp.where(lane0, -sr, ci - sr))
            keep_ref[2, part] = jnp.where(row0, sr, jnp.where(lane0, ci, cr - si))
            keep_ref[3, part] = jnp.where(row0, si, jnp.where(lane0, -si, ci + sr))
        else:
            keep_ref[0, part] = jnp.where(lane0, cr, cr + si)
            keep_ref[1, part] = jnp.where(lane0, -sr, ci - sr)
            keep_ref[2, part] = jnp.where(lane0, ci, cr - si)
            keep_ref[3, part] = jnp.where(lane0, -si, ci + sr)
    block = rows // shots

    def give(order, target):
        owner = lax.rem(shot_ref[0] + 2 * shots - way * (1 + order), shots)
        part = pl.ds(pl.multiple_of(owner * block, 8), block)
        target[0, :block] = keep_ref[0, part]
        target[1, :block] = keep_ref[1, part]
        target[0, block:] = keep_ref[2, part]
        target[1, block:] = keep_ref[3, part]

    @pl.when(step < per_way)
    def _():
        give(0, up_ref.at[0])

    @pl.when(step >= per_way)
    def _():
        give(0, down_ref.at[0])

    for order in range(1, shots):
        give(order, rest_ref.at[order - 1, 0])


def plane_terms(weights, shot, source, receivers, model, tables, shots, first, count):
    _, planes, width_y, width_x = source.shape
    members = receivers.shape[0]
    x_values, y_values = tables
    whole = lambda a: pl.BlockSpec(a.shape, lambda p: (0,) * a.ndim)
    piece = (2, width_y // shots, width_x // 2)
    return pl.pallas_call(
        functools.partial(plane_kernel, shots, first),
        grid=(count,),
        in_specs=[
            pl.BlockSpec(memory_space=pltpu.SMEM),
            pl.BlockSpec(memory_space=pltpu.SMEM),
            pl.BlockSpec((1, 1, width_y, width_x), lambda p: (0, p + first, 0, 0)),
            pl.BlockSpec((members, 1, width_y, width_x), lambda p: (0, p + first, 0, 0)),
            whole(model),
            whole(x_values),
            whole(y_values),
        ],
        out_specs=[
            pl.BlockSpec((1,) + piece, lambda p: (jnp.minimum(p, count // 2 - 1), 0, 0, 0)),
            pl.BlockSpec((1,) + piece, lambda p: (jnp.maximum(p - count // 2, 0), 0, 0, 0)),
            pl.BlockSpec((shots - 1, 1) + piece, lambda p: (0, p, 0, 0, 0)),
        ],
        out_shape=[
            jax.ShapeDtypeStruct((count // 2,) + piece, F32),
            jax.ShapeDtypeStruct((count // 2,) + piece, F32),
            jax.ShapeDtypeStruct((shots - 1, count) + piece, F32),
        ],
        scratch_shapes=[pltpu.VMEM((4, width_y // 2, width_x // 2), F32)],
        cost_estimate=pl.CostEstimate(
            flops=count * 3 * width_y * width_x * (width_x + width_y),
            bytes_accessed=count * 10 * width_y * width_x,
            transcendentals=0,
        ),
        name="plane_terms",
        interpret=INTERPRET,
    )(weights, shot, source, receivers, model, x_values, y_values)


def plane_lines(chunks, ins, c, slot, h):
    lanes = slice(h * LANES, (h + 1) * LANES)
    parts = []
    for q, came in enumerate(ins[:chunks]):
        last = ins[chunks + q // 2]
        count = came.shape[0]
        parts.append(came[:, c, slot, lanes] + last[0, (q % 2) * count : (q % 2 + 1) * count, c, slot, lanes])
    return jnp.concatenate(parts, axis=0)


def power_kernel(chunks, shot_ref, *refs):
    ins, out_ref = refs[:-1], refs[-1]
    planes = sum(ref.shape[0] for ref in ins[:chunks])
    _, _, slots, half = ins[0].shape
    halves_x = half // LANES
    first = shot_ref[0] == 0
    lane0 = lax.broadcasted_iota(jnp.int32, (1, LANES), 1) == 0
    pos = [jnp.zeros((planes, LANES), F32) for _ in range(halves_x)]
    neg = [jnp.zeros((planes, LANES), F32) for _ in range(halves_x)]
    fix_a = jnp.zeros((planes, LANES), F32)
    fix_b = jnp.zeros((planes, LANES), F32)
    for slot in range(slots):
        for h in range(halves_x):
            real = plane_lines(chunks, ins, 0, slot, h)
            imag = plane_lines(chunks, ins, 1, slot, h)
            real2, imag2 = real * real, imag * imag
            energy = real2 + imag2
            if h == 0 and slot in (0, slots // 2):
                fix_a = fix_a + real2
                fix_b = fix_b + imag2
                energy = jnp.where(lane0 & first, 0.0, energy)
            if slot < slots // 2:
                pos[h] = pos[h] + energy
            else:
                neg[h] = neg[h] + energy
    keep = first.astype(F32)
    lines = []
    for side, fix in ((pos, fix_a), (neg, fix_b)):
        for h in range(halves_x):
            total = pos[h] + neg[h]
            lines.append(jnp.where(lane0, 2.0 * side[0] + keep * fix, total) if h == 0 else total)
    sums = jnp.concatenate([jnp.sum(line, axis=0, keepdims=True) for line in lines], axis=0)
    sums = jnp.concatenate([sums, jnp.zeros((8 - sums.shape[0], LANES), F32)], axis=0)
    for peer in range(out_ref.shape[0]):
        out_ref[peer] = sums


def pack_kernel(groups, chunks, power_ref, *refs):
    ins, out_ref = refs[:-1], refs[-1]
    planes = sum(ref.shape[0] for ref in ins[:chunks])
    _, _, slots, half = ins[0].shape
    rows = slots // groups
    for slot in range(slots):
        g, r = divmod(slot, rows)
        for h in range(half // LANES):
            d = h * groups + g
            for c in range(2):
                start = (c * rows + r) * planes
                out_ref[d, start : start + planes] = plane_lines(chunks, ins, c, slot, h)
    power = jnp.sum(power_ref[...], axis=0)
    base = 2 * rows * planes
    for d in range(out_ref.shape[0]):
        out_ref[d, base:] = power


def over_rings(kernel, name, lead, lead_spec, came, rests, out_shape):
    return pl.pallas_call(
        functools.partial(kernel, len(came)),
        grid=(1,),
        in_specs=[lead_spec]
        + [pl.BlockSpec(a.shape, lambda i: (0, 0, 0, 0)) for a in came]
        + [pl.BlockSpec((1,) + a.shape[1:], lambda i, last=a.shape[0] - 1: (last, 0, 0, 0, 0)) for a in rests],
        out_specs=pl.BlockSpec(out_shape, lambda i: (0, 0, 0)),
        out_shape=jax.ShapeDtypeStruct(out_shape, F32),
        cost_estimate=pl.CostEstimate(flops=10**9, bytes_accessed=10**6, transcendentals=0),
        compiler_params=ROOM,
        name=name,
        interpret=INTERPRET,
    )(lead, *came, *rests)


def levels_of(power, sizes, scales, cells):
    wedges = sizes.shape[1]
    down = lax.broadcasted_iota(jnp.int32, (wedges, wedges), 0)
    across = lax.broadcasted_iota(jnp.int32, (wedges, wedges), 1)
    size_row = jnp.broadcast_to(sizes.astype(F32), (wedges, wedges))
    scale_row = jnp.broadcast_to(scales, (wedges, wedges))
    ends = jnp.sum(jnp.where(across <= down, size_row, 0.0), axis=1, keepdims=True)
    size = jnp.sum(jnp.where(across == down, size_row, 0.0), axis=1, keepdims=True)
    scale = jnp.sum(jnp.where(across == down, scale_row, 0.0), axis=1, keepdims=True)
    starts = ends - size
    half_lines = power.shape[0] // 2
    half = half_lines * LANES
    members = []
    total = jnp.zeros((wedges, 1), F32)
    for line in range(2 * half_lines):
        column = half_lines * lax.broadcasted_iota(jnp.int32, (wedges, LANES), 1) + line % half_lines
        if line >= half_lines:
            column = jnp.where(column == 0, half, 2 * half - column)
        column = column.astype(F32)
        member = (column >= starts) & (column < ends)
        members.append(member)
        total = total + jnp.sum(jnp.where(member, power[line : line + 1], 0.0), axis=1, keepdims=True)
    spread = jnp.sqrt(total / (size * cells) + EPSILON)
    level = scale * spread
    return [jnp.sum(jnp.where(member, level, 0.0), axis=0, keepdims=True) for member in members]


def depth_kernel(in_ref, z_ref, out_ref, power_ref):
    sources, message, _ = in_ref.shape
    depth = z_ref.shape[2]
    planes = depth // sources
    pieces = []
    for start in range(0, message - 8, planes):
        pieces.append(in_ref[:, start : start + planes, :].reshape(depth, LANES))
    out_ref[...] = dot3((z_ref[0], z_ref[1]), split(jnp.concatenate(pieces, axis=1)))
    power_ref[...] = jnp.sum(in_ref[:, message - 8 :, :], axis=0)


def along_depth(received, tables):
    vmem = pl.BlockSpec(memory_space=pltpu.VMEM)
    planes = tables.shape[2] // received.shape[0]
    wide = (received.shape[1] - 8) // planes * LANES
    return pl.pallas_call(
        depth_kernel,
        in_specs=[vmem] * 2,
        out_specs=[vmem] * 2,
        out_shape=[
            jax.ShapeDtypeStruct((tables.shape[1], wide), F32),
            jax.ShapeDtypeStruct((8, LANES), F32),
        ],
        cost_estimate=pl.CostEstimate(flops=4 * 10**9, bytes_accessed=3 * 10**6, transcendentals=0),
        compiler_params=ROOM,
        name="along_depth",
        interpret=INTERPRET,
    )(received, tables)


def shrink_kernel(
    groups, slabs, cells, place_ref, both_ref, power_ref, sizes_ref, scales_ref, z_ref, out_ref
):
    depth = z_ref.shape[2]
    rows = both_ref.shape[1] // (2 * LANES)
    shot, slab = place_ref[0], place_ref[1]
    h, g = slab // groups, slab % groups
    lines = levels_of(power_ref[: 2 * (slabs // groups)] * depth, sizes_ref[...], scales_ref[...], cells)
    half_lines = len(lines) // 2
    own, mirror = lines[0], lines[half_lines]
    for other in range(1, half_lines):
        own = jnp.where(h == other, lines[other], own)
        mirror = jnp.where(h == other, lines[half_lines + other], mirror)
    lane = lax.broadcasted_iota(jnp.int32, (1, LANES), 1)
    edge = (lane == 0) & (h == 0)
    level_zero, level_mid = lines[0], lines[half_lines]
    upper = g >= groups // 2
    edge_level = jnp.where(upper, level_mid, level_zero)
    one = jnp.where(edge, edge_level, own)
    two = jnp.where(edge, edge_level, mirror)
    packed_here = (shot == 0) & (h == 0) & ((g == 0) | (g == groups // 2))
    packed = (lane == 0) & packed_here
    table = (z_ref[0], z_ref[1])
    shrunk_r, shrunk_i = [], []
    for r in range(rows):
        real = slice(r * LANES, (r + 1) * LANES)
        imag = slice((rows + r) * LANES, (rows + r + 1) * LANES)
        cr, sr = both_ref[:depth, real], both_ref[depth:, real]
        ci, si = both_ref[:depth, imag], both_ref[depth:, imag]
        zr, zi = cr + si, ci - sr
        energy = zr * zr + zi * zi
        if r == 0:
            energy_a = jnp.where(packed, cr * cr + sr * sr, energy)
            energy_b = jnp.where(packed, ci * ci + si * si, energy)
            one_a = jnp.where(packed, level_zero, one)
            two_a = jnp.where(packed, level_zero, two)
            one_b = jnp.where(packed, level_mid, one)
            two_b = jnp.where(packed, level_mid, two)
            factor_a = mean_factor(energy_a, one_a, two_a)
            factor_b = mean_factor(energy_b, one_b, two_b)
            shrunk_r.append(factor_a * cr + factor_b * si)
            shrunk_i.append(factor_b * ci - factor_a * sr)
        else:
            factor = mean_factor(energy, one, two)
            shrunk_r.append(factor * zr)
            shrunk_i.append(factor * zi)
    back = dot3(table, split(jnp.concatenate(shrunk_r + shrunk_i, axis=1)))
    wide = rows * LANES
    out_ref[:, 0, :wide] = back[:depth, :wide] - back[depth:, wide:]
    out_ref[:, 0, wide:] = back[:depth, wide:] + back[depth:, :wide]


def mean_factor(energy, one, two):
    magnitude = jnp.sqrt(energy)
    first = jnp.maximum(magnitude - one, 0.0) / jnp.maximum(magnitude, one)
    second = jnp.maximum(magnitude - two, 0.0) / jnp.maximum(magnitude, two)
    return 0.5 * (first + second)


def shrink(place, both, power, sizes, scales, tables, groups, slabs, cells):
    depth, wide = tables.shape[2], both.shape[1]
    vmem = pl.BlockSpec(memory_space=pltpu.VMEM)
    return pl.pallas_call(
        functools.partial(shrink_kernel, groups, slabs, float(cells)),
        in_specs=[pl.BlockSpec(memory_space=pltpu.SMEM)] + [vmem] * 5,
        out_specs=vmem,
        out_shape=jax.ShapeDtypeStruct((depth, 1, wide), F32),
        compiler_params=ROOM,
        name="shrink",
        interpret=INTERPRET,
    )(place, both, power, sizes, scales, tables)


def image_kernel(groups, scale, in_ref, back_ref, x_ref, out_ref):
    count, _, wide = in_ref.shape
    rows = wide // (2 * LANES)
    halves_x = x_ref.shape[1]
    per_half = count // halves_x
    mid = per_half // 2
    row = lax.broadcasted_iota(jnp.int32, (mid, LANES), 0)
    lane = lax.broadcasted_iota(jnp.int32, (mid, LANES), 1)
    columns = [[], []]
    for h in range(halves_x):
        cos_r, cos_i, sin_r, sin_i = [], [], [], []
        for r in range(rows):
            real = slice(r * LANES, (r + 1) * LANES)
            imag = slice((rows + r) * LANES, (rows + r + 1) * LANES)
            low = slice(h * per_half, h * per_half + mid)
            high = slice(h * per_half + mid, (h + 1) * per_half)
            pr, pi = in_ref[low, 0, real], in_ref[low, 0, imag]
            nr, ni = in_ref[high, 0, real], in_ref[high, 0, imag]
            cr, ci, sr, si = pr + nr, pi + ni, ni - pi, pr - nr
            if h == 0:
                lane0 = lane == 0
                cr = jnp.where(lane0, 2.0 * pr, cr)
                ci = jnp.where(lane0, 2.0 * nr, ci)
                sr = jnp.where(lane0, -2.0 * pi, sr)
                si = jnp.where(lane0, -2.0 * ni, si)
            if r == 0:
                row0 = row == 0
                cr = jnp.where(row0, pr, cr)
                ci = jnp.where(row0, pi, ci)
                sr = jnp.where(row0, nr, sr)
                si = jnp.where(row0, ni, si)
            cos_r.append(cr)
            cos_i.append(ci)
            sin_r.append(sr)
            sin_i.append(si)
        columns[0].append(jnp.concatenate(cos_r + sin_r, axis=0))
        columns[1].append(jnp.concatenate(cos_i + sin_i, axis=0))
    stacked = jnp.concatenate(columns[0] + columns[1], axis=1)
    along_y = dot3((back_ref[0], back_ref[1]), split(stacked))
    lanes = lax.broadcasted_iota(jnp.int32, (1, along_y.shape[1]), 1)
    single = (lanes == 0) | (lanes == along_y.shape[1] // 2)
    along_y = along_y * jnp.where(single, scale, 2.0 * scale)
    high, low = split(along_y)
    half = along_y.shape[1] // 2
    parts = []
    for h in range(halves_x):
        own = slice(h * LANES, (h + 1) * LANES)
        other = slice(half + h * LANES, half + (h + 1) * LANES)
        value = [jnp.concatenate([a[:, own], a[:, other]], axis=1) for a in (high, low)]
        parts.append(dot3(value, (x_ref[0, h], x_ref[1, h]), (((1,), (1,)), ((), ()))))
    out_ref[0, :, :half] = parts[0] + parts[1]
    out_ref[0, :, half:] = parts[0] - parts[1]


def image_of(returned, back_tables, x_tables, groups, scale, shape):
    vmem = pl.BlockSpec(memory_space=pltpu.VMEM)
    return pl.pallas_call(
        functools.partial(image_kernel, groups, scale),
        in_specs=[vmem] * 3,
        out_specs=vmem,
        out_shape=jax.ShapeDtypeStruct(shape, F32),
        compiler_params=ROOM,
        name="image",
        interpret=INTERPRET,
    )(returned, back_tables, x_tables)


def exchange(pieces, axes):
    return lax.all_to_all(pieces, axes, split_axis=0, concat_axis=0, tiled=True)


def on_device(source_field, receiver_fields, weights, model, wedge_sizes, wedge_scales):
    planes, width_y, width_x = source_field.shape[1:]
    shots = lax.axis_size("shot")
    slabs = lax.axis_size(SLAB)
    depth = planes * slabs
    groups = slabs // (width_x // 2 // LANES)
    rows = width_y // shots // groups
    shot = lax.axis_index("shot").astype(jnp.int32)
    slab = lax.axis_index(SLAB).astype(jnp.int32)
    x_tables = halves(x_table(width_x))
    y_tables = halves(y_table(width_y))
    z_tables = halves(z_table(depth))
    back_tables = halves(y_back_table(width_y, shots, groups // 2, rows))
    chunk = planes // (CHUNKS // 2)
    came, rests = [], []
    for q in range(CHUNKS // 2):
        up, down, rest = plane_terms(
            weights, shot[None], source_field, receiver_fields, model, (x_tables, y_tables), shots, q * chunk, chunk
        )
        came += [up, down]
        rests.append(rest)
    half = chunk // 2
    for step in range(shots - 1):
        for q in range(CHUNKS):
            way = 1 - 2 * (q % 2)
            moved = lax.ppermute(came[q], "shot", [(i, (i + way) % shots) for i in range(shots)])
            if step < shots - 2:
                moved = moved + rests[q // 2][step, (q % 2) * half : (q % 2 + 1) * half]
            came[q] = moved
    smem = pl.BlockSpec(memory_space=pltpu.SMEM)
    power_shape = (shots, 8, LANES)
    power = over_rings(power_kernel, "power", shot[None], smem, came, rests, power_shape)
    power = exchange(power, "shot")
    message = over_rings(
        functools.partial(pack_kernel, groups), "pack", power, pl.BlockSpec(power_shape, lambda i: (0, 0, 0)),
        came, rests, (slabs, 2 * rows * planes + 8, LANES),
    )
    both, power = along_depth(exchange(message, SLAB), z_tables)
    shrunk = shrink(
        jnp.stack([shot, slab]),
        both,
        power,
        wedge_sizes[None],
        wedge_scales[None],
        z_tables,
        groups,
        slabs,
        depth * width_y,
    )
    returned = exchange(shrunk, SLAB_SHOT)
    scale = 1.0 / (depth * width_y * width_x)
    return image_of(returned, back_tables, x_tables, groups, scale, model.shape)


def solution(mesh):
    torus = Mesh(
        mesh.devices.reshape(mesh.shape["shot"], 4, 4, 2), ("shot", "slab_0", "slab_1", "slab_2")
    )
    return jax.shard_map(
        on_device,
        mesh=torus,
        in_specs=(
            P("shot", SLAB, None, None),
            P("shot", SLAB, None, None),
            P("shot"),
            P(SLAB_SHOT, None, None),
            P(),
            P(),
        ),
        out_specs=P(SLAB_SHOT, None, None),
        check_vma=False,
    )
```

```python
import functools

import jax
import jax.numpy as jnp
import numpy as np
from jax import lax
from jax.experimental import pallas as pl
from jax.experimental.pallas import tpu as pltpu
from jax.sharding import Mesh
from jax.sharding import PartitionSpec as P

SLAB = ("slab_0", "slab_1", "slab_2")
SLAB_SHOT = ("slab_0", "slab_1", "slab_2", "shot")

STEP_SIZE = 0.25
EPSILON = 1e-06
LANES = 128
F32 = jnp.float32
BF16 = jnp.bfloat16
INTERPRET = False
CHUNKS = 4
ROOM = pltpu.CompilerParams(vmem_limit_bytes=24 * 1024 * 1024)


def halves(table):
    high = np.asarray(table, dtype=np.float32).astype(jnp.bfloat16)
    low = (np.asarray(table) - high.astype(np.float64)).astype(np.float32).astype(jnp.bfloat16)
    return jnp.asarray(np.stack([high, low]))


def angles(rows, columns, length):
    return 2.0 * np.pi * (np.outer(rows, columns) % length) / length


def x_table(width):
    half = width // 2
    tables = []
    for h in range(2):
        angle = angles(np.arange(half), np.arange(h, half, 2), width)
        sine = -np.sin(angle)
        if h == 0:
            sine[:, 0] = 1.0 - 2.0 * (np.arange(half) % 2)
        tables.append(np.concatenate([np.cos(angle), sine], axis=1))
    return np.stack(tables)


def y_order(width):
    half = width // 2
    return np.concatenate([np.arange(0, half, 2), np.arange(1, half, 2)])


def y_rows(width, length):
    angle = angles(y_order(width), np.arange(length), width)
    sine = np.sin(angle)
    sine[0] = 1.0 - 2.0 * (np.arange(length) % 2)
    return np.cos(angle), sine


def y_table(width):
    cos, sin = y_rows(width, width // 2)
    quarter = width // 4
    return np.stack(
        [np.concatenate([cos[part], sin[part]]) for part in (slice(0, quarter), slice(quarter, None))]
    )


def y_back_table(width, shots, parts, rows):
    half = width // 2
    r, g, j = np.meshgrid(np.arange(rows), np.arange(parts), np.arange(shots), indexing="ij")
    slot = (j * (half // shots) + g * rows + r).reshape(-1)
    cos, sin = y_rows(width, width)
    return np.concatenate([cos[slot].T, sin[slot].T], axis=1)


def z_table(depth):
    angle = angles(np.arange(depth), np.arange(depth), depth)
    return np.concatenate([np.cos(angle), np.sin(angle)], axis=0)


def split(value):
    high = value.astype(BF16)
    low = (value - high.astype(F32)).astype(BF16)
    return high, low


def dot(a, b, dims=(((1,), (0,)), ((), ()))):
    return lax.dot_general(a, b, dims, preferred_element_type=F32)


def dot3(a, b, dims=(((1,), (0,)), ((), ()))):
    return dot(a[0], b[0], dims) + (dot(a[1], b[0], dims) + dot(a[0], b[1], dims))


def plane_kernel(
    shots, first, weight_ref, shot_ref, source_ref, receiver_ref, model_ref, x_ref, y_ref,
    up_ref, down_ref, rest_ref, keep_ref
):
    step = pl.program_id(0)
    plane = step + first
    per_way = pl.num_programs(0) // 2
    way = jnp.where(step < per_way, 1, -1)
    members = receiver_ref.shape[0]
    own = (plane == shot_ref[0]).astype(F32)
    width_y, width_x = source_ref.shape[2:]
    rows, half = width_y // 2, width_x // 2
    encoded = weight_ref[0].astype(F32) * receiver_ref[0, 0].astype(F32)
    for member in range(1, members):
        encoded = encoded + weight_ref[member].astype(F32) * receiver_ref[member, 0].astype(F32)
    term = source_ref[0, 0].astype(F32) * encoded
    term = own * model_ref[0].astype(F32) - STEP_SIZE * term
    low, high = term[:, :half], term[:, half:]
    cosines, sines = [], []
    for h, fold in ((0, low + high), (1, low - high)):
        fold = jnp.concatenate([fold[:rows] + fold[rows:], fold[:rows] - fold[rows:]], axis=0)
        along_x = dot3(split(fold), (x_ref[0, h], x_ref[1, h]))
        cosines.append(along_x[:, : half // 2])
        sines.append(along_x[:, half // 2 :])
    along_x = jnp.concatenate(cosines + sines, axis=1)
    quarter = rows // 2
    row = lax.broadcasted_iota(jnp.int32, (quarter, half), 0)
    lane0 = lax.broadcasted_iota(jnp.int32, (quarter, half), 1) == 0
    for parity in range(2):
        both = dot3((y_ref[0, parity], y_ref[1, parity]), split(along_x[parity * rows : (parity + 1) * rows]))
        cr, ci = both[:quarter, :half], both[:quarter, half:]
        sr, si = both[quarter:, :half], both[quarter:, half:]
        part = pl.ds(parity * quarter, quarter)
        if parity == 0:
            row0 = row == 0
            keep_ref[0, part] = jnp.where(row0 | lane0, cr, cr + si)
            keep_ref[1, part] = jnp.where(row0, ci, jnp.where(lane0, -sr, ci - sr))
            keep_ref[2, part] = jnp.where(row0, sr, jnp.where(lane0, ci, cr - si))
            keep_ref[3, part] = jnp.where(row0, si, jnp.where(lane0, -si, ci + sr))
        else:
            keep_ref[0, part] = jnp.where(lane0, cr, cr + si)
            keep_ref[1, part] = jnp.where(lane0, -sr, ci - sr)
            keep_ref[2, part] = jnp.where(lane0, ci, cr - si)
            keep_ref[3, part] = jnp.where(lane0, -si, ci + sr)
    block = rows // shots

    def give(order, target):
        owner = lax.rem(shot_ref[0] + 2 * shots - way * (1 + order), shots)
        part = pl.ds(pl.multiple_of(owner * block, 8), block)
        target[0, :block] = keep_ref[0, part]
        target[1, :block] = keep_ref[1, part]
        target[0, block:] = keep_ref[2, part]
        target[1, block:] = keep_ref[3, part]

    @pl.when(step < per_way)
    def _():
        give(0, up_ref.at[0])

    @pl.when(step >= per_way)
    def _():
        give(0, down_ref.at[0])

    for order in range(1, shots):
        give(order, rest_ref.at[order - 1, 0])


def plane_terms(weights, shot, source, receivers, model, tables, shots, first, count):
    _, planes, width_y, width_x = source.shape
    members = receivers.shape[0]
    x_values, y_values = tables
    whole = lambda a: pl.BlockSpec(a.shape, lambda p: (0,) * a.ndim)
    piece = (2, width_y // shots, width_x // 2)
    return pl.pallas_call(
        functools.partial(plane_kernel, shots, first),
        grid=(count,),
        in_specs=[
            pl.BlockSpec(memory_space=pltpu.SMEM),
            pl.BlockSpec(memory_space=pltpu.SMEM),
            pl.BlockSpec((1, 1, width_y, width_x), lambda p: (0, p + first, 0, 0)),
            pl.BlockSpec((members, 1, width_y, width_x), lambda p: (0, p + first, 0, 0)),
            whole(model),
            whole(x_values),
            whole(y_values),
        ],
        out_specs=[
            pl.BlockSpec((1,) + piece, lambda p: (jnp.minimum(p, count // 2 - 1), 0, 0, 0)),
            pl.BlockSpec((1,) + piece, lambda p: (jnp.maximum(p - count // 2, 0), 0, 0, 0)),
            pl.BlockSpec((shots - 1, 1) + piece, lambda p: (0, p, 0, 0, 0)),
        ],
        out_shape=[
            jax.ShapeDtypeStruct((count // 2,) + piece, F32),
            jax.ShapeDtypeStruct((count // 2,) + piece, F32),
            jax.ShapeDtypeStruct((shots - 1, count) + piece, F32),
        ],
        scratch_shapes=[pltpu.VMEM((4, width_y // 2, width_x // 2), F32)],
        cost_estimate=pl.CostEstimate(
            flops=count * 3 * width_y * width_x * (width_x + width_y),
            bytes_accessed=count * 10 * width_y * width_x,
            transcendentals=0,
        ),
        name="plane_terms",
        interpret=INTERPRET,
    )(weights, shot, source, receivers, model, x_values, y_values)


def plane_lines(chunks, ins, c, slot, h):
    lanes = slice(h * LANES, (h + 1) * LANES)
    parts = []
    for q, came in enumerate(ins[:chunks]):
        last = ins[chunks + q // 2]
        count = came.shape[0]
        parts.append(came[:, c, slot, lanes] + last[0, (q % 2) * count : (q % 2 + 1) * count, c, slot, lanes])
    return jnp.concatenate(parts, axis=0)


def power_kernel(chunks, shot_ref, *refs):
    ins, out_ref = refs[:-1], refs[-1]
    planes = sum(ref.shape[0] for ref in ins[:chunks])
    _, _, slots, half = ins[0].shape
    halves_x = half // LANES
    first = shot_ref[0] == 0
    lane0 = lax.broadcasted_iota(jnp.int32, (1, LANES), 1) == 0
    pos = [jnp.zeros((planes, LANES), F32) for _ in range(halves_x)]
    neg = [jnp.zeros((planes, LANES), F32) for _ in range(halves_x)]
    fix_a = jnp.zeros((planes, LANES), F32)
    fix_b = jnp.zeros((planes, LANES), F32)
    for slot in range(slots):
        for h in range(halves_x):
            real = plane_lines(chunks, ins, 0, slot, h)
            imag = plane_lines(chunks, ins, 1, slot, h)
            real2, imag2 = real * real, imag * imag
            energy = real2 + imag2
            if h == 0 and slot in (0, slots // 2):
                fix_a = fix_a + real2
                fix_b = fix_b + imag2
                energy = jnp.where(lane0 & first, 0.0, energy)
            if slot < slots // 2:
                pos[h] = pos[h] + energy
            else:
                neg[h] = neg[h] + energy
    keep = first.astype(F32)
    lines = []
    for side, fix in ((pos, fix_a), (neg, fix_b)):
        for h in range(halves_x):
            total = pos[h] + neg[h]
            lines.append(jnp.where(lane0, 2.0 * side[0] + keep * fix, total) if h == 0 else total)
    sums = jnp.concatenate([jnp.sum(line, axis=0, keepdims=True) for line in lines], axis=0)
    sums = jnp.concatenate([sums, jnp.zeros((8 - sums.shape[0], LANES), F32)], axis=0)
    for peer in range(out_ref.shape[0]):
        out_ref[peer] = sums


def pack_kernel(groups, chunks, power_ref, *refs):
    ins, out_ref = refs[:-1], refs[-1]
    planes = sum(ref.shape[0] for ref in ins[:chunks])
    _, _, slots, half = ins[0].shape
    rows = slots // groups
    for slot in range(slots):
        g, r = divmod(slot, rows)
        for h in range(half // LANES):
            d = h * groups + g
            for c in range(2):
                start = (c * rows + r) * planes
                out_ref[d, start : start + planes] = plane_lines(chunks, ins, c, slot, h)
    power = jnp.sum(power_ref[...], axis=0)
    base = 2 * rows * planes
    for d in range(out_ref.shape[0]):
        out_ref[d, base:] = power


def over_rings(kernel, name, lead, lead_spec, came, rests, out_shape):
    return pl.pallas_call(
        functools.partial(kernel, len(came)),
        grid=(1,),
        in_specs=[lead_spec]
        + [pl.BlockSpec(a.shape, lambda i: (0, 0, 0, 0)) for a in came]
        + [pl.BlockSpec((1,) + a.shape[1:], lambda i, last=a.shape[0] - 1: (last, 0, 0, 0, 0)) for a in rests],
        out_specs=pl.BlockSpec(out_shape, lambda i: (0, 0, 0)),
        out_shape=jax.ShapeDtypeStruct(out_shape, F32),
        cost_estimate=pl.CostEstimate(flops=10**9, bytes_accessed=10**6, transcendentals=0),
        compiler_params=ROOM,
        name=name,
        interpret=INTERPRET,
    )(lead, *came, *rests)


def levels_of(power, sizes, scales, cells):
    wedges = sizes.shape[1]
    down = lax.broadcasted_iota(jnp.int32, (wedges, wedges), 0)
    across = lax.broadcasted_iota(jnp.int32, (wedges, wedges), 1)
    size_row = jnp.broadcast_to(sizes.astype(F32), (wedges, wedges))
    scale_row = jnp.broadcast_to(scales, (wedges, wedges))
    ends = jnp.sum(jnp.where(across <= down, size_row, 0.0), axis=1, keepdims=True)
    size = jnp.sum(jnp.where(across == down, size_row, 0.0), axis=1, keepdims=True)
    scale = jnp.sum(jnp.where(across == down, scale_row, 0.0), axis=1, keepdims=True)
    starts = ends - size
    half_lines = power.shape[0] // 2
    half = half_lines * LANES
    members = []
    total = jnp.zeros((wedges, 1), F32)
    for line in range(2 * half_lines):
        column = half_lines * lax.broadcasted_iota(jnp.int32, (wedges, LANES), 1) + line % half_lines
        if line >= half_lines:
            column = jnp.where(column == 0, half, 2 * half - column)
        column = column.astype(F32)
        member = (column >= starts) & (column < ends)
        members.append(member)
        total = total + jnp.sum(jnp.where(member, power[line : line + 1], 0.0), axis=1, keepdims=True)
    spread = jnp.sqrt(total / (size * cells) + EPSILON)
    level = scale * spread
    return [jnp.sum(jnp.where(member, level, 0.0), axis=0, keepdims=True) for member in members]


def depth_kernel(in_ref, z_ref, out_ref, power_ref):
    sources, message, _ = in_ref.shape
    depth = z_ref.shape[2]
    planes = depth // sources
    pieces = []
    for start in range(0, message - 8, planes):
        pieces.append(in_ref[:, start : start + planes, :].reshape(depth, LANES))
    out_ref[...] = dot3((z_ref[0], z_ref[1]), split(jnp.concatenate(pieces, axis=1)))
    power_ref[...] = jnp.sum(in_ref[:, message - 8 :, :], axis=0)


def along_depth(received, tables):
    vmem = pl.BlockSpec(memory_space=pltpu.VMEM)
    planes = tables.shape[2] // received.shape[0]
    wide = (received.shape[1] - 8) // planes * LANES
    return pl.pallas_call(
        depth_kernel,
        in_specs=[vmem] * 2,
        out_specs=[vmem] * 2,
        out_shape=[
            jax.ShapeDtypeStruct((tables.shape[1], wide), F32),
            jax.ShapeDtypeStruct((8, LANES), F32),
        ],
        cost_estimate=pl.CostEstimate(flops=4 * 10**9, bytes_accessed=3 * 10**6, transcendentals=0),
        compiler_params=ROOM,
        name="along_depth",
        interpret=INTERPRET,
    )(received, tables)


def shrink_kernel(
    groups, slabs, cells, place_ref, both_ref, power_ref, sizes_ref, scales_ref, z_ref, out_ref
):
    depth = z_ref.shape[2]
    rows = both_ref.shape[1] // (2 * LANES)
    shot, slab = place_ref[0], place_ref[1]
    h, g = slab // groups, slab % groups
    lines = levels_of(power_ref[: 2 * (slabs // groups)] * depth, sizes_ref[...], scales_ref[...], cells)
    half_lines = len(lines) // 2
    own, mirror = lines[0], lines[half_lines]
    for other in range(1, half_lines):
        own = jnp.where(h == other, lines[other], own)
        mirror = jnp.where(h == other, lines[half_lines + other], mirror)
    lane = lax.broadcasted_iota(jnp.int32, (1, LANES), 1)
    edge = (lane == 0) & (h == 0)
    level_zero, level_mid = lines[0], lines[half_lines]
    upper = g >= groups // 2
    edge_level = jnp.where(upper, level_mid, level_zero)
    one = jnp.where(edge, edge_level, own)
    two = jnp.where(edge, edge_level, mirror)
    packed_here = (shot == 0) & (h == 0) & ((g == 0) | (g == groups // 2))
    packed = (lane == 0) & packed_here
    table = (z_ref[0], z_ref[1])
    shrunk_r, shrunk_i = [], []
    for r in range(rows):
        real = slice(r * LANES, (r + 1) * LANES)
        imag = slice((rows + r) * LANES, (rows + r + 1) * LANES)
        cr, sr = both_ref[:depth, real], both_ref[depth:, real]
        ci, si = both_ref[:depth, imag], both_ref[depth:, imag]
        zr, zi = cr + si, ci - sr
        energy = zr * zr + zi * zi
        if r == 0:
            energy_a = jnp.where(packed, cr * cr + sr * sr, energy)
            energy_b = jnp.where(packed, ci * ci + si * si, energy)
            one_a = jnp.where(packed, level_zero, one)
            two_a = jnp.where(packed, level_zero, two)
            one_b = jnp.where(packed, level_mid, one)
            two_b = jnp.where(packed, level_mid, two)
            factor_a = mean_factor(energy_a, one_a, two_a)
            factor_b = mean_factor(energy_b, one_b, two_b)
            shrunk_r.append(factor_a * cr + factor_b * si)
            shrunk_i.append(factor_b * ci - factor_a * sr)
        else:
            factor = mean_factor(energy, one, two)
            shrunk_r.append(factor * zr)
            shrunk_i.append(factor * zi)
    back = dot3(table, split(jnp.concatenate(shrunk_r + shrunk_i, axis=1)))
    wide = rows * LANES
    out_ref[:, 0, :wide] = back[:depth, :wide] - back[depth:, wide:]
    out_ref[:, 0, wide:] = back[:depth, wide:] + back[depth:, :wide]


def mean_factor(energy, one, two):
    magnitude = jnp.sqrt(energy)
    first = jnp.maximum(magnitude - one, 0.0) / jnp.maximum(magnitude, one)
    second = jnp.maximum(magnitude - two, 0.0) / jnp.maximum(magnitude, two)
    return 0.5 * (first + second)


def shrink(place, both, power, sizes, scales, tables, groups, slabs, cells):
    depth, wide = tables.shape[2], both.shape[1]
    vmem = pl.BlockSpec(memory_space=pltpu.VMEM)
    return pl.pallas_call(
        functools.partial(shrink_kernel, groups, slabs, float(cells)),
        in_specs=[pl.BlockSpec(memory_space=pltpu.SMEM)] + [vmem] * 5,
        out_specs=vmem,
        out_shape=jax.ShapeDtypeStruct((depth, 1, wide), F32),
        compiler_params=ROOM,
        name="shrink",
        interpret=INTERPRET,
    )(place, both, power, sizes, scales, tables)


def image_kernel(groups, scale, in_ref, back_ref, x_ref, out_ref):
    count, _, wide = in_ref.shape
    rows = wide // (2 * LANES)
    halves_x = x_ref.shape[1]
    per_half = count // halves_x
    mid = per_half // 2
    row = lax.broadcasted_iota(jnp.int32, (mid, LANES), 0)
    lane = lax.broadcasted_iota(jnp.int32, (mid, LANES), 1)
    columns = [[], []]
    for h in range(halves_x):
        cos_r, cos_i, sin_r, sin_i = [], [], [], []
        for r in range(rows):
            real = slice(r * LANES, (r + 1) * LANES)
            imag = slice((rows + r) * LANES, (rows + r + 1) * LANES)
            low = slice(h * per_half, h * per_half + mid)
            high = slice(h * per_half + mid, (h + 1) * per_half)
            pr, pi = in_ref[low, 0, real], in_ref[low, 0, imag]
            nr, ni = in_ref[high, 0, real], in_ref[high, 0, imag]
            cr, ci, sr, si = pr + nr, pi + ni, ni - pi, pr - nr
            if h == 0:
                lane0 = lane == 0
                cr = jnp.where(lane0, 2.0 * pr, cr)
                ci = jnp.where(lane0, 2.0 * nr, ci)
                sr = jnp.where(lane0, -2.0 * pi, sr)
                si = jnp.where(lane0, -2.0 * ni, si)
            if r == 0:
                row0 = row == 0
                cr = jnp.where(row0, pr, cr)
                ci = jnp.where(row0, pi, ci)
                sr = jnp.where(row0, nr, sr)
                si = jnp.where(row0, ni, si)
            cos_r.append(cr)
            cos_i.append(ci)
            sin_r.append(sr)
            sin_i.append(si)
        columns[0].append(jnp.concatenate(cos_r + sin_r, axis=0))
        columns[1].append(jnp.concatenate(cos_i + sin_i, axis=0))
    stacked = jnp.concatenate(columns[0] + columns[1], axis=1)
    along_y = dot3((back_ref[0], back_ref[1]), split(stacked))
    lanes = lax.broadcasted_iota(jnp.int32, (1, along_y.shape[1]), 1)
    single = (lanes == 0) | (lanes == along_y.shape[1] // 2)
    along_y = along_y * jnp.where(single, scale, 2.0 * scale)
    high, low = split(along_y)
    half = along_y.shape[1] // 2
    parts = []
    for h in range(halves_x):
        own = slice(h * LANES, (h + 1) * LANES)
        other = slice(half + h * LANES, half + (h + 1) * LANES)
        value = [jnp.concatenate([a[:, own], a[:, other]], axis=1) for a in (high, low)]
        parts.append(dot3(value, (x_ref[0, h], x_ref[1, h]), (((1,), (1,)), ((), ()))))
    out_ref[0, :, :half] = parts[0] + parts[1]
    out_ref[0, :, half:] = parts[0] - parts[1]


def image_of(returned, back_tables, x_tables, groups, scale, shape):
    vmem = pl.BlockSpec(memory_space=pltpu.VMEM)
    return pl.pallas_call(
        functools.partial(image_kernel, groups, scale),
        in_specs=[vmem] * 3,
        out_specs=vmem,
        out_shape=jax.ShapeDtypeStruct(shape, F32),
        compiler_params=ROOM,
        name="image",
        interpret=INTERPRET,
    )(returned, back_tables, x_tables)


def exchange(pieces, axes):
    return lax.all_to_all(pieces, axes, split_axis=0, concat_axis=0, tiled=True)


def on_device(source_field, receiver_fields, weights, model, wedge_sizes, wedge_scales):
    planes, width_y, width_x = source_field.shape[1:]
    shots = lax.axis_size("shot")
    slabs = lax.axis_size(SLAB)
    depth = planes * slabs
    groups = slabs // (width_x // 2 // LANES)
    rows = width_y // shots // groups
    shot = lax.axis_index("shot").astype(jnp.int32)
    slab = lax.axis_index(SLAB).astype(jnp.int32)
    place = jnp.stack([shot, slab])
    x_tables = halves(x_table(width_x))
    y_tables = halves(y_table(width_y))
    z_tables = halves(z_table(depth))
    back_tables = halves(y_back_table(width_y, shots, groups // 2, rows))
    chunk = planes // (CHUNKS // 2)
    came, rests = [], []
    for q in range(CHUNKS // 2):
        up, down, rest = plane_terms(
            weights, place, source_field, receiver_fields, model, (x_tables, y_tables), shots, q * chunk, chunk
        )
        came += [up, down]
        rests.append(rest)
    half = chunk // 2
    for step in range(shots - 1):
        for q in range(CHUNKS):
            way = 1 - 2 * (q % 2)
            moved = lax.ppermute(came[q], "shot", [(i, (i + way) % shots) for i in range(shots)])
            if step < shots - 2:
                moved = moved + rests[q // 2][step, (q % 2) * half : (q % 2 + 1) * half]
            came[q] = moved
    smem = pl.BlockSpec(memory_space=pltpu.SMEM)
    power_shape = (shots, 8, LANES)
    power = over_rings(power_kernel, "power", place, smem, came, rests, power_shape)
    power = exchange(power, "shot")
    message = over_rings(
        functools.partial(pack_kernel, groups), "pack", power, pl.BlockSpec(power_shape, lambda i: (0, 0, 0)),
        came, rests, (slabs, 2 * rows * planes + 8, LANES),
    )
    both, power = along_depth(exchange(message, SLAB), z_tables)
    shrunk = shrink(
        place,
        both,
        power,
        wedge_sizes[None],
        wedge_scales[None],
        z_tables,
        groups,
        slabs,
        depth * width_y,
    )
    returned = exchange(shrunk, SLAB_SHOT)
    scale = 1.0 / (depth * width_y * width_x)
    return image_of(returned, back_tables, x_tables, groups, scale, model.shape)


def solution(mesh):
    torus = Mesh(
        mesh.devices.reshape(mesh.shape["shot"], 4, 4, 2), ("shot", "slab_0", "slab_1", "slab_2")
    )
    return jax.shard_map(
        on_device,
        mesh=torus,
        in_specs=(
            P("shot", SLAB, None, None),
            P("shot", SLAB, None, None),
            P("shot"),
            P(SLAB_SHOT, None, None),
            P(),
            P(),
        ),
        out_specs=P(SLAB_SHOT, None, None),
        check_vma=False,
    )
```
